128 devices in a mesh: block: 4 (over x), tok: 32 (over z, y, core).
Axes of the slice: x: 4, y: 4, z: 4, core: 2. Of those that a mesh axis runs over, the one named last changes fastest.
Arguments:
- keys: bfloat16 [4, 2, 8192, 1280], P('block', None, 'tok'), may hold values from -6 to 6
- values: bfloat16 [4, 2, 8192, 1280], P('block', None, 'tok'), may hold values from -6 to 6
- queries: bfloat16 [4, 2, 8192, 1280], P('block', None, 'tok'), may hold values from -6 to 6
- rates: bfloat16 [4, 2, 8192, 20], P('block', None, 'tok'), may hold values from 0.00049972534 to 0.0049743652
- counts: int32 [4, 2, 32, 20], P('block', None, 'tok'), may hold values from 1 to 256
- stagger: int32 [20], replicated, may hold values from 0 to 255
- gate_in: bfloat16 [4, 20, 64, 512], P('block', None, None, 'tok'), may hold values from -0.75 to 0.75
- up_in: bfloat16 [4, 20, 64, 512], P('block', None, None, 'tok'), may hold values from -0.75 to 0.75
- down_in: bfloat16 [4, 20, 64, 512], P('block', None, None, 'tok'), may hold values from -0.25 to 0.25
- entry_gate: bfloat16 [20, 64, 512], replicated, may hold values from -0.75 to 0.75
- entry_up: bfloat16 [20, 64, 512], replicated, may hold values from -0.75 to 0.75
- entry_down: bfloat16 [20, 64, 512], replicated, may hold values from -0.25 to 0.25
Outputs:
- answers: bfloat16 [4, 2, 8192, 1280], P('block', None, 'tok')
- gate_out: bfloat16 [4, 20, 64, 512], P('block', None, None, 'tok')
- up_out: bfloat16 [4, 20, 64, 512], P('block', None, None, 'tok')
- down_out: bfloat16 [4, 20, 64, 512], P('block', None, None, 'tok')
The draws below stay inside these ranges and needn't reach their ends.
All inputs are finite; a program needn't handle non-finite values.
Results may differ from the reference program's by a relative error of at most 0.022.
Values may be sent and summed in bfloat16 or wider, within the bound.
No kernel may reach another device: no remote copies, remote signals or barrier semaphores. Data moves between devices by JAX's collectives and lax.ppermute only.
A program may use at most 320 MiB of HBM per device.

```python
import math
import jax
import jax.numpy as jnp
from jax import lax

HEADS = 20
DH = 64
FH = 512
ROWS = 256
TICKS = 2
NCHUNK = 4
TOKS = 8192
N_TOK = 32


def touch_ends(values, own_key, low, high):
    dims = values.shape
    spot = [jax.random.randint(jax.random.fold_in(own_key, axis), (), 0, dims[axis]) for axis in range(len(dims))]
    values = values.at[tuple(spot)].set(low)
    longest = dims.index(max(dims))
    spot[longest] = (spot[longest] + 1) % dims[longest]
    return values.at[tuple(spot)].set(high)


def steps_of(key, extent, shards, least, top_value):
    loudness, own = 1.0, jax.random.fold_in(key, 6)
    for dim, blocks in shards:
        draws = jnp.exp(jax.random.uniform(jax.random.fold_in(own, dim), (blocks,), jnp.float32, least / len(shards), top_value / len(shards)))
        loudness = loudness * jnp.repeat(draws, extent[dim] // blocks).reshape([-1 if axis == dim else 1 for axis in range(len(extent))])
    return loudness


def centred(own_key, extent, scale, most, shards=(), held_as=jnp.bfloat16):
    values = scale * jax.random.normal(own_key, extent, jnp.float32)
    if shards:
        values = values * steps_of(own_key, extent, shards, -0.22, 0.18)
    return jnp.clip(values, -most, most).astype(held_as)


def setup_inputs(seed: int = 0) -> dict:
    key_of = jax.random.split(jax.random.key(seed), 13)
    return {
        "keys": centred(key_of[0], (NCHUNK, TICKS, TOKS, HEADS * DH), 1.0, 6.0, ((0, 4), (2, 32))),
        "values": centred(key_of[1], (NCHUNK, TICKS, TOKS, HEADS * DH), 1.0, 6.0, ((0, 4), (2, 32))),
        "queries": centred(key_of[2], (NCHUNK, TICKS, TOKS, HEADS * DH), 1.0, 6.0, ((0, 4), (2, 32))),
        "rates": jnp.clip(jnp.exp(math.log(0.0049743652) - 2.2979944 * jax.random.uniform(key_of[3], (NCHUNK, TICKS, TOKS, HEADS), jnp.float32) ** steps_of(key_of[3], (NCHUNK, TICKS, TOKS, HEADS), ((0, 4), (2, 32)), -0.2, 0.2)), 0.00049972534, 0.0049743652).astype(jnp.bfloat16),
        "counts": touch_ends(jax.random.randint(key_of[4], (NCHUNK, TICKS, N_TOK, HEADS), 1, ROWS + 1), jax.random.fold_in(key_of[4], 1), 1, ROWS).astype(jnp.int32),
        "stagger": touch_ends(jax.random.randint(key_of[5], (HEADS,), 0, ROWS), jax.random.fold_in(key_of[5], 1), 0, ROWS - 1).astype(jnp.int32),
        "gate_in": centred(key_of[6], (NCHUNK, HEADS, DH, FH), DH ** -0.5, 0.75, ((0, 4), (3, 32))),
        "up_in": centred(key_of[7], (NCHUNK, HEADS, DH, FH), DH ** -0.5, 0.75, ((0, 4), (3, 32))),
        "down_in": centred(key_of[8], (NCHUNK, HEADS, DH, FH), FH ** -0.5, 0.25, ((0, 4), (3, 32))),
        "entry_gate": centred(key_of[9], (HEADS, DH, FH), DH ** -0.5, 0.75),
        "entry_up": centred(key_of[10], (HEADS, DH, FH), DH ** -0.5, 0.75),
        "entry_down": centred(key_of[11], (HEADS, DH, FH), FH ** -0.5, 0.25),
    }


EPS = 1e-06

def gradients(keys, values, scale, weights):
    gate_w, up_w, down_w = weights
    rows = keys.shape[0]
    heads = gate_w.shape[0]
    size = gate_w.shape[1]
    kk = keys.reshape(rows, heads, size).astype(jnp.float32)
    vv = values.reshape(rows, heads, size).astype(jnp.float32)
    pre_gate = jnp.einsum('rhd,hdf->rhf', kk, gate_w.astype(jnp.float32))
    pre_up = jnp.einsum('rhd,hdf->rhf', kk, up_w.astype(jnp.float32))
    back = jnp.einsum('rhd,hdf->rhf', vv, down_w.astype(jnp.float32))
    weight = scale.astype(jnp.float32)[:, :, None]
    sig = jax.nn.sigmoid(pre_gate)
    act = pre_gate * sig
    hidden = (weight * act * pre_up).astype(jnp.bfloat16)
    d_gate = (weight * back * pre_up * sig * (1.0 + pre_gate * (1.0 - sig))).astype(jnp.bfloat16)
    d_up = (weight * back * act).astype(jnp.bfloat16)
    step_gate = jnp.einsum('rhd,rhf->hdf', kk, d_gate.astype(jnp.float32))
    step_up = jnp.einsum('rhd,rhf->hdf', kk, d_up.astype(jnp.float32))
    step_down = jnp.einsum('rhd,rhf->hdf', vv, hidden.astype(jnp.float32))
    return (step_gate, step_up, step_down)

def renew(weights, steps):
    result = []
    for weight, step in zip(weights, steps):
        base = weight.astype(jnp.float32)
        moved = base + step
        before = jnp.sqrt(lax.optimization_barrier(jnp.sum(base * base, axis=1, keepdims=True)) + EPS)
        after = jnp.sqrt(lax.optimization_barrier(jnp.sum(moved * moved, axis=1, keepdims=True)) + EPS)
        result.append((moved * (before / after)).astype(jnp.bfloat16))
    return tuple(result)

def respond(queries, weights):
    gate_w, up_w, down_w = weights
    rows = queries.shape[0]
    heads = gate_w.shape[0]
    size = gate_w.shape[1]
    qq = queries.reshape(rows, heads, size).astype(jnp.float32)
    pre_gate = jnp.einsum('rhd,hdf->rhf', qq, gate_w.astype(jnp.float32))
    pre_up = jnp.einsum('rhd,hdf->rhf', qq, up_w.astype(jnp.float32))
    hidden = (jax.nn.silu(pre_gate) * pre_up).astype(jnp.bfloat16)
    output = jnp.einsum('rhf,hdf->rhd', hidden.astype(jnp.float32), down_w.astype(jnp.float32))
    return output.reshape(rows, heads * size)

def reference(keys, values, queries, rates, counts, stagger, gate_in, up_in, down_in, entry_gate, entry_up, entry_down):
    index = jnp.arange(TOKS, dtype=jnp.int32)
    shard = index // ROWS
    offset = index % ROWS
    inside = jnp.mod(offset[:, None] - stagger[None, :].astype(jnp.int32), ROWS)

    def one_tick(items):
        kk, vv, qq, rr, cc, g_w, u_w, d_w = items
        limit = cc[shard, :]
        scale = jnp.where(inside < limit, rr, jnp.zeros_like(rr))
        weights = (g_w, u_w, d_w)
        steps = gradients(kk, vv, scale, weights)
        renewed = renew(weights, steps)
        return (respond(qq, renewed).astype(jnp.bfloat16), renewed)
    first, mid = lax.map(one_tick, (keys[:, 0], values[:, 0], queries[:, 0], rates[:, 0], counts[:, 0], gate_in, up_in, down_in))
    entries = (entry_gate, entry_up, entry_down)
    carried = tuple((jnp.concatenate([e[None], m[:-1]], axis=0) for e, m in zip(entries, mid)))
    second, final = lax.map(one_tick, (keys[:, 1], values[:, 1], queries[:, 1], rates[:, 1], counts[:, 1], carried[0], carried[1], carried[2]))
    answers = jnp.stack([first, second], axis=1)
    return (answers, final[0], final[1], final[2])
```

```python
import jax
import jax.numpy as jnp
from jax import lax
from jax.experimental import pallas as pl
from jax.experimental.pallas import tpu as pltpu
from jax.sharding import PartitionSpec as P

EPS = 1e-06
BF = jnp.bfloat16
F32 = jnp.float32

HEADS = 20
DH = 64
FH = 512
ROWS = 256
NTOK = 32
UNITS = FH // NTOK
PAIRS = HEADS // 2
EDGE = 176
MID = ROWS - EDGE
SUB = 16
TILE = 256
PER = TILE // SUB
SHARE = 2 * UNITS
IN_ROWS = 224
OUT_ROWS = EDGE + SHARE
LIST = NTOK * EDGE // SUB
UPS = [(3 * g + a, 3 * g + a + 1) for g in range(PAIRS) for a in (0, 1)]
DOWNS = [(3 * g + a + 1, 3 * g + a) for g in range(PAIRS) for a in (0, 1)]


def low_lanes(shape):
    return lax.broadcasted_iota(jnp.int32, shape, 1) < DH


def swap(x):
    return pltpu.roll(x.astype(F32), DH, 1).astype(x.dtype)


def pair_up(left, right):
    low = low_lanes(left.shape)
    return jnp.where(low, left, swap(right)), jnp.where(low, swap(left), right)


def scatter_rows(out_ref, g, first, second):
    out_ref[3 * g, 0:EDGE] = first[0:EDGE]
    out_ref[3 * g + 1, 0:MID] = first[EDGE:ROWS]
    out_ref[3 * g + 1, MID : 2 * MID] = second[0:MID]
    out_ref[3 * g + 2, 0:EDGE] = second[MID:ROWS]


def scaled_values(values_ref, rates_ref, counts_ref, stagger_ref, tick):
    offset = lax.broadcasted_iota(jnp.int32, (ROWS, HEADS), 0)
    inside = (offset - stagger_ref[...] + ROWS) & (ROWS - 1)
    scale = jnp.where(inside < counts_ref[tick], rates_ref[tick].astype(F32), 0.0).astype(BF)
    owner = lax.broadcasted_iota(jnp.int32, (HEADS, HEADS * DH), 1) // DH
    spread = (owner == lax.broadcasted_iota(jnp.int32, (HEADS, HEADS * DH), 0)).astype(F32).astype(BF)
    wide = jnp.dot(scale, spread, preferred_element_type=F32)
    return (values_ref[tick].astype(F32) * wide).astype(BF)


def eye(n):
    same = lax.broadcasted_iota(jnp.int32, (n, n), 0) == lax.broadcasted_iota(jnp.int32, (n, n), 1)
    return same.astype(F32).astype(BF)


def turned(share):
    return lax.dot_general(eye(UNITS), share, (((1,), (1,)), ((), ())), preferred_element_type=F32).astype(BF)


def pack_first(keys_ref, values_ref, rates_ref, counts_ref, stagger_ref, gate_ref, up_ref, down_ref, out_ref):
    scaled = scaled_values(values_ref, rates_ref, counts_ref, stagger_ref, 0)
    keys = keys_ref[0]
    gate, up, down = turned(gate_ref[...]), turned(up_ref[...]), turned(down_ref[...])
    zero = jnp.zeros((UNITS, 2 * DH), BF)
    out_ref[3 * PAIRS :] = jnp.zeros((NTOK - 3 * PAIRS, IN_ROWS, 2 * DH), BF)
    for g in range(PAIRS):
        lanes = slice(2 * DH * g, 2 * DH * (g + 1))
        first, second = pair_up(keys[:, lanes], scaled[:, lanes])
        scatter_rows(out_ref, g, first, second)
        shares = []
        for gu, w in zip(pair_up(gate[:, lanes], up[:, lanes]), pair_up(zero, down[:, lanes])):
            shares.append(jnp.concatenate([gu, w], axis=0))
        out_ref[3 * g, EDGE : EDGE + SHARE] = shares[0]
        out_ref[3 * g + 1, 2 * MID : 2 * MID + SHARE] = shares[0]
        out_ref[3 * g + 1, 2 * MID + SHARE : 2 * MID + 2 * SHARE] = shares[1]
        out_ref[3 * g + 2, EDGE : EDGE + SHARE] = shares[1]
        for d in (0, 2):
            out_ref[3 * g + d, EDGE + SHARE :] = jnp.zeros((IN_ROWS - EDGE - SHARE, 2 * DH), BF)


def finish_rows(out_ref):
    out_ref[3 * PAIRS :] = jnp.zeros((NTOK - 3 * PAIRS, EDGE, 2 * DH), BF)
    for g in range(PAIRS):
        out_ref[3 * g + 1, 2 * MID :] = jnp.zeros((EDGE - 2 * MID, 2 * DH), BF)


def pack_second(keys_ref, values_ref, rates_ref, counts_ref, stagger_ref, out_ref):
    scaled = scaled_values(values_ref, rates_ref, counts_ref, stagger_ref, 1)
    keys = keys_ref[1]
    finish_rows(out_ref)
    for g in range(PAIRS):
        lanes = slice(2 * DH * g, 2 * DH * (g + 1))
        scatter_rows(out_ref, g, *pair_up(keys[:, lanes], scaled[:, lanes]))


def pack_queries(queries_ref, out_ref):
    finish_rows(out_ref)
    for g in range(PAIRS):
        lanes = slice(2 * DH * g, 2 * DH * (g + 1))
        scatter_rows(out_ref, g, *pair_up(queries_ref[0, :, lanes], queries_ref[1, :, lanes]))


def whole_weights(role_ref, rows_ref, out_ref):
    role = role_ref[0]

    def of(start):
        gu = jnp.concatenate([rows_ref[s, pl.ds(start, UNITS)] for s in range(NTOK)], axis=0)
        w = jnp.concatenate([rows_ref[s, pl.ds(start + UNITS, UNITS)] for s in range(NTOK)], axis=0)
        gu = gu.astype(F32).T.astype(BF)
        w = w.astype(F32).T.astype(BF)
        return jnp.concatenate([gu[:DH], gu[DH:], w[DH:]], axis=1)

    start = pl.multiple_of(jnp.where(role == 1, 2 * MID, EDGE), SUB)
    out_ref[0] = of(start)
    start = pl.multiple_of(jnp.where(role == 1, 2 * MID + SHARE, EDGE), SUB)
    out_ref[1] = of(start)


def slot_bounds(role, slot):
    if slot == 0:
        return 0, jnp.where(role == 0, EDGE // SUB, jnp.where(role == 1, MID // SUB, 0))
    return (
        jnp.where(role == 1, MID // SUB, 0),
        jnp.where(role == 2, EDGE // SUB, jnp.where(role == 1, MID // SUB, 0)),
    )


def fill_list(list_ref, role, slot):
    begin, blocks = slot_bounds(role, slot)

    def per_shard(s, n):
        def per_block(j, n):
            list_ref[n] = s * 16 + begin + j
            return n + 1

        return lax.fori_loop(0, blocks, per_block, n)

    count = lax.fori_loop(0, NTOK, per_shard, jnp.int32(0))

    def pad(j, c):
        list_ref[count + j] = 0
        return c

    lax.fori_loop(0, PER, pad, 0)
    return count


def block_at(ref, entry):
    return ref[entry // 16, pl.ds(pl.multiple_of((entry % 16) * SUB, SUB), SUB)]


def gradient(role_ref, rows_ref, weights_ref, own_ref, up_ref, down_ref, stack, acc, list_ref):
    role = role_ref[0]
    zero = jnp.zeros((DH, FH), BF)
    for slot in range(2):
        w = weights_ref[slot]
        half = (w[:, :FH].astype(F32) * 0.5).astype(BF)
        stack[:DH] = jnp.concatenate([half, w[:, FH : 2 * FH], zero], axis=1)
        stack[DH:] = jnp.concatenate([zero, zero, w[:, 2 * FH :]], axis=1)
        acc[...] = jnp.zeros((DH, 3 * FH), F32)
        count = fill_list(list_ref, role, slot)

        def step(i, c):
            base = i * PER
            kv = jnp.concatenate([block_at(rows_ref, list_ref[base + j]) for j in range(PER)], axis=0)
            row = lax.broadcasted_iota(jnp.int32, (TILE, 2 * DH), 0)
            kv = jnp.where(row < (count - base) * SUB, kv.astype(F32), 0.0).astype(BF)
            turn = kv.astype(F32).T.astype(BF)
            k_t, v_t = turn[:DH], turn[DH:]
            width = 256
            for f in range(0, FH, width):
                half_gate = jnp.dot(kv, stack[:, f : f + width], preferred_element_type=F32)
                up = jnp.dot(kv, stack[:, FH + f : FH + f + width], preferred_element_type=F32)
                back = jnp.dot(kv, stack[:, 2 * FH + f : 2 * FH + f + width], preferred_element_type=F32)
                twice = jnp.tanh(half_gate) + 1.0
                act = half_gate * twice
                sig = 0.5 * twice
                slope = sig + act * (1.0 - sig)
                hidden = (act * up).astype(BF)
                d_gate = (back * up * slope).astype(BF)
                d_up = (back * act).astype(BF)
                acc[:, f : f + width] += jnp.dot(k_t, d_gate, preferred_element_type=F32)
                acc[:, FH + f : FH + f + width] += jnp.dot(k_t, d_up, preferred_element_type=F32)
                acc[:, 2 * FH + f : 2 * FH + f + width] += jnp.dot(v_t, hidden, preferred_element_type=F32)
            return c

        lax.fori_loop(0, (count + PER - 1) // PER, step, 0)
        own_ref[slot] = acc[...].astype(BF)
    up_ref[...] = own_ref[jnp.where(role == 0, 0, 1)]
    down_ref[...] = own_ref[jnp.where(role == 1, 0, 1)]


def renew(role_ref, weights_ref, own_ref, below_ref, above_ref, out_ref):
    role = role_ref[0]
    below, above = below_ref[...].astype(F32), above_ref[...].astype(F32)
    others = (jnp.where(role == 0, above, below), jnp.where(role == 1, above, below))
    for slot in range(2):
        base = weights_ref[slot].astype(F32)
        moved = base + (own_ref[slot].astype(F32) + others[slot])
        before = jnp.sum(base * base, axis=0, keepdims=True) + EPS
        after = jnp.sum(moved * moved, axis=0, keepdims=True) + EPS
        out_ref[slot] = (moved * (jnp.sqrt(before) / jnp.sqrt(after))).astype(BF)


def respond(tick):
    def kernel(role_ref, rows_ref, weights_ref, *refs):
        if tick == 0:
            out_ref, stack, list_ref = refs
        else:
            prev_ref, out_ref, stack, list_ref = refs
        role = role_ref[0]
        zero = jnp.zeros((DH, 2 * FH), BF)
        at = slice(0, DH) if tick == 0 else slice(DH, 2 * DH)
        off = slice(DH, 2 * DH) if tick == 0 else slice(0, DH)
        if tick == 0:
            out_ref[...] = jnp.zeros(out_ref.shape, BF)
        else:
            for s in range(NTOK):
                out_ref[s, 2 * MID : EDGE] = jnp.zeros((EDGE - 2 * MID, 2 * DH), BF)
        for slot in range(2):
            w = weights_ref[slot]
            half = (w[:, :FH].astype(F32) * 0.5).astype(BF)
            stack[at] = jnp.concatenate([half, w[:, FH : 2 * FH]], axis=1)
            stack[off] = zero
            nothing = jnp.zeros((DH, FH), F32)
            down = w[:, 2 * FH :].astype(F32)
            down = jnp.concatenate([down, nothing] if tick == 0 else [nothing, down], axis=0).T.astype(BF)
            count = fill_list(list_ref, role, slot)

            def step(i, c):
                base = i * PER
                q = jnp.concatenate([block_at(rows_ref, list_ref[base + j]) for j in range(PER)], axis=0)
                total = None
                width = 256
                for f in range(0, FH, width):
                    half_gate = jnp.dot(q, stack[:, f : f + width], preferred_element_type=F32)
                    up = jnp.dot(q, stack[:, FH + f : FH + f + width], preferred_element_type=F32)
                    hidden = (half_gate * (jnp.tanh(half_gate) + 1.0) * up).astype(BF)
                    part = jnp.dot(hidden, down[f : f + width], preferred_element_type=F32)
                    total = part if total is None else total + part
                answer = total.astype(BF)
                for j in range(PER):
                    entry = list_ref[base + j]
                    piece = answer[j * SUB : (j + 1) * SUB]
                    if tick == 1:
                        piece = jnp.where(low_lanes(piece.shape), block_at(prev_ref, entry), piece)
                    out_ref[entry // 16, pl.ds(pl.multiple_of((entry % 16) * SUB, SUB), SUB)] = piece
                return c

            lax.fori_loop(0, count // PER, step, 0)
        if tick == 1:
            w = jnp.where(role == 0, weights_ref[0].astype(F32), weights_ref[1].astype(F32))
            gu = jnp.concatenate([w[:, :FH], w[:, FH : 2 * FH]], axis=0).T.astype(BF)
            dn = jnp.concatenate([jnp.zeros((DH, FH), F32), w[:, 2 * FH :]], axis=0).T.astype(BF)
            for s in range(NTOK):
                out_ref[s, EDGE : EDGE + UNITS] = gu[s * UNITS : (s + 1) * UNITS]
                out_ref[s, EDGE + UNITS :] = dn[s * UNITS : (s + 1) * UNITS]

    return kernel


def unpack(rows_ref, answers_ref, gate_ref, up_ref, down_ref):
    gates, ups, downs = [], [], []
    for g in range(PAIRS):
        lanes = slice(2 * DH * g, 2 * DH * (g + 1))
        first = jnp.concatenate([rows_ref[3 * g, 0:EDGE], rows_ref[3 * g + 1, 0:MID]], axis=0)
        second = jnp.concatenate([rows_ref[3 * g + 1, MID : 2 * MID], rows_ref[3 * g + 2, 0:EDGE]], axis=0)
        tick0, tick1 = pair_up(first, second)
        answers_ref[0, :, lanes] = tick0
        answers_ref[1, :, lanes] = tick1
        one, two = rows_ref[3 * g, EDGE:], rows_ref[3 * g + 2, EDGE:]
        gate, up = pair_up(one[:UNITS], two[:UNITS])
        _, down = pair_up(one[UNITS:], two[UNITS:])
        gates.append(gate)
        ups.append(up)
        downs.append(down)
    for ref, parts in ((gate_ref, gates), (up_ref, ups), (down_ref, downs)):
        whole = jnp.concatenate(parts, axis=1)
        ref[...] = lax.dot_general(whole, eye(UNITS), (((0,), (0,)), ((), ())), preferred_element_type=F32).astype(BF)


def call(kernel, name, outs, args, scalars=0, scratch=()):
    spec = lambda: pl.BlockSpec(memory_space=pltpu.VMEM)
    many = isinstance(outs, (tuple, list))
    return pl.pallas_call(
        kernel,
        name=name,
        out_shape=outs,
        in_specs=[pl.BlockSpec(memory_space=pltpu.SMEM)] * scalars + [spec() for _ in args[scalars:]],
        out_specs=tuple(spec() for _ in outs) if many else spec(),
        scratch_shapes=list(scratch),
        compiler_params=pltpu.CompilerParams(vmem_limit_bytes=56 * 1024 * 1024),
    )(*args)


def shape(*dims):
    return jax.ShapeDtypeStruct(dims, BF)


def exchange(rows):
    result = lax.all_to_all(rows.reshape(-1, 2 * DH), "tok", split_axis=0, concat_axis=0, tiled=True)
    return result.reshape(rows.shape)


def shards(keys, values, queries, rates, counts, stagger, gate_in, up_in, down_in, entry_gate, entry_up, entry_down):
    me = lax.axis_index("tok")
    role = jnp.where(me < 3 * PAIRS, me % 3, 3).astype(jnp.int32)[None]
    pair = jnp.minimum(me // 3, PAIRS - 1)
    keys, values, queries, rates, counts = (a[0] for a in (keys, values, queries, rates, counts))
    stagger = stagger[None, :]
    shares = [w[0].reshape(HEADS * DH, UNITS) for w in (gate_in, up_in, down_in)]

    packed = call(
        pack_first,
        "pack_first",
        shape(NTOK, IN_ROWS, 2 * DH),
        (keys, values, rates, counts, stagger, *shares),
    )
    rows0 = exchange(packed)
    rows1 = exchange(
        call(pack_second, "pack_second", shape(NTOK, EDGE, 2 * DH), (keys, values, rates, counts, stagger))
    )
    rows_q = exchange(call(pack_queries, "pack_queries", shape(NTOK, EDGE, 2 * DH), (queries,)))
    entries = jnp.concatenate(
        [lax.dynamic_slice_in_dim(e, 2 * pair, 2, 0) for e in (entry_gate, entry_up, entry_down)], axis=2
    )

    weight = shape(DH, 3 * FH)
    weights = shape(2, DH, 3 * FH)
    lists = pltpu.SMEM((LIST + 2 * PER,), jnp.int32)

    def tick(rows, current):
        own, up, down = call(
            gradient,
            "gradient",
            (weights, weight, weight),
            (role, rows, current),
            1,
            (pltpu.VMEM((2 * DH, 3 * FH), BF), pltpu.VMEM((DH, 3 * FH), F32), lists),
        )
        below = lax.ppermute(up, "tok", UPS)
        above = lax.ppermute(down, "tok", DOWNS)
        return call(renew, "renew", weights, (role, current, own, below, above), 1)

    current = call(whole_weights, "whole_weights", weights, (role, rows0), 1)
    first = tick(rows0, current)
    size = lax.axis_size("block")
    passed = lax.ppermute(first, "block", [(b, b + 1) for b in range(size - 1)])
    second = tick(rows1, jnp.where(lax.axis_index("block") == 0, entries, passed))

    scratch = (pltpu.VMEM((2 * DH, 2 * FH), BF), lists)
    answers0 = call(respond(0), "respond_first", shape(NTOK, EDGE, 2 * DH), (role, rows_q, first), 1, scratch)
    packed = call(
        respond(1), "respond_second", shape(NTOK, OUT_ROWS, 2 * DH), (role, rows_q, second, answers0), 1, scratch
    )
    answers, gate, up, down = call(
        unpack,
        "unpack",
        (shape(2, ROWS, HEADS * DH),) + (shape(HEADS * DH, UNITS),) * 3,
        (exchange(packed),),
    )
    return (answers[None], *(w.reshape(1, HEADS, DH, UNITS) for w in (gate, up, down)))


def solution(mesh):
    tokens = P("block", None, "tok", None)
    share = P("block", None, None, "tok")
    return jax.shard_map(
        shards,
        mesh=mesh,
        in_specs=(tokens,) * 5 + (P(),) + (share,) * 3 + (P(),) * 3,
        out_specs=(tokens, share, share, share),
        check_vma=False,
    )
```

```python
import jax
import jax.numpy as jnp
from jax import lax
from jax.experimental import pallas as pl
from jax.experimental.pallas import tpu as pltpu
from jax.sharding import PartitionSpec as P


EPS = 1e-06
BF = jnp.bfloat16
F32 = jnp.float32

HEADS = 20
DH = 64
FH = 512
ROWS = 256
NTOK = 32
UNITS = FH // NTOK
PAIRS = HEADS // 2
EDGE = 176
MID = ROWS - EDGE
SUB = 16
TILE = 512
SHARE = 2 * UNITS
IN_ROWS = 224
HALF = EDGE // 2
OUT_ROWS = 2 * HALF + SHARE
WIDTH = 256
PIECE = 256
PACKED = NTOK * EDGE + TILE
UPS = [(3 * g + a, 3 * g + a + 1) for g in range(PAIRS) for a in (0, 1)]
DOWNS = [(3 * g + a + 1, 3 * g + a) for g in range(PAIRS) for a in (0, 1)]


def low_lanes(shape):
    return lax.broadcasted_iota(jnp.int32, shape, 1) < DH


def swap(x):
    return pltpu.roll(x.astype(F32), DH, 1).astype(x.dtype)


def pair_up(left, right):
    low = low_lanes(left.shape)
    return jnp.where(low, left, swap(right)), jnp.where(low, swap(left), right)


def scatter_rows(out_ref, g, first, second):
    out_ref[3 * g, 0:EDGE] = first[0:EDGE]
    out_ref[3 * g + 1, 0:MID] = first[EDGE:ROWS]
    out_ref[3 * g + 1, MID : 2 * MID] = second[0:MID]
    out_ref[3 * g + 2, 0:EDGE] = second[MID:ROWS]


def spread_of():
    owner = lax.broadcasted_iota(jnp.int32, (HEADS, HEADS * DH), 1) // DH
    return (owner == lax.broadcasted_iota(jnp.int32, (HEADS, HEADS * DH), 0)).astype(F32).astype(BF)


def scaled_values(values, rates_ref, counts_ref, stagger_ref, tick):
    offset = lax.broadcasted_iota(jnp.int32, (1, ROWS), 1)
    scale = []
    for h in range(HEADS):
        inside = (offset - stagger_ref[h] + ROWS) & (ROWS - 1)
        scale.append(jnp.where(inside < counts_ref[tick, h], rates_ref[h, tick : tick + 1].astype(F32), 0.0))
    scale = jnp.concatenate(scale, axis=0).astype(BF)
    wide = lax.dot_general(scale, spread_of(), (((0,), (0,)), ((), ())), preferred_element_type=F32)
    return (values.astype(F32) * wide).astype(BF)


def pack_first(
    counts_ref, stagger_ref, keys_hbm, values_hbm, rates_hbm, gate_hbm, up_hbm, down_hbm, out_hbm,
    keys_ref, values_ref, rates_ref, gate_ref, up_ref, down_ref, out_ref, loads, stores,
):
    pairs = (
        (rates_hbm, rates_ref),
        (values_hbm.at[0], values_ref),
        (keys_hbm.at[0], keys_ref),
        (gate_hbm, gate_ref),
        (up_hbm, up_ref),
        (down_hbm, down_ref),
    )
    copies = [pltpu.make_async_copy(src, dst, loads.at[n]) for n, (src, dst) in enumerate(pairs)]
    for copy in copies:
        copy.start()
    out_ref[3 * PAIRS :] = jnp.zeros((NTOK - 3 * PAIRS, IN_ROWS, 2 * DH), BF)
    for g in range(PAIRS):
        for d in (0, 2):
            out_ref[3 * g + d, EDGE + SHARE :] = jnp.zeros((IN_ROWS - EDGE - SHARE, 2 * DH), BF)
    for copy in copies:
        copy.wait()
    scaled = scaled_values(values_ref[...], rates_ref, counts_ref, stagger_ref, 0)

    def share(h):
        half = (UNITS // 2, DH)
        counts = [jnp.full(half, counts_ref[t, h].astype(F32), F32) for t in range(2)]
        gu = jnp.concatenate([gate_ref[h], up_ref[h]], axis=1)
        w = jnp.concatenate([jnp.concatenate(counts, axis=0).astype(BF), down_ref[h]], axis=1)
        return jnp.concatenate([gu, w], axis=0)

    sent = []
    for g in range(PAIRS + 1):
        lo, n = 3 * g, 3 if g < PAIRS else NTOK - 3 * PAIRS
        if g < PAIRS:
            lanes = slice(2 * DH * g, 2 * DH * (g + 1))
            first, second = pair_up(keys_ref[:, lanes], scaled[:, lanes])
            scatter_rows(out_ref, g, first, second)
            shares = share(2 * g), share(2 * g + 1)
            out_ref[3 * g, EDGE : EDGE + SHARE] = shares[0]
            out_ref[3 * g + 1, 2 * MID : 2 * MID + SHARE] = shares[0]
            out_ref[3 * g + 1, 2 * MID + SHARE : 2 * MID + 2 * SHARE] = shares[1]
            out_ref[3 * g + 2, EDGE : EDGE + SHARE] = shares[1]
        sent.append(pltpu.make_async_copy(out_ref.at[pl.ds(lo, n)], out_hbm.at[pl.ds(lo, n)], stores.at[g]))
        sent[-1].start()
    for copy in sent:
        copy.wait()


def pack_queries(queries, out_ref, at):
    out_ref[3 * PAIRS :, at : at + HALF] = jnp.zeros((NTOK - 3 * PAIRS, HALF, 2 * DH), BF)
    for g in range(PAIRS):
        tile = queries[:, 2 * DH * g : 2 * DH * (g + 1)].astype(F32)
        turn = pltpu.roll(tile, DH, 1)
        low = low_lanes((HALF, 2 * DH))
        out_ref[3 * g, at : at + HALF] = jnp.where(low, tile[:HALF], turn[HALF:EDGE]).astype(BF)
        middle = jnp.where(low_lanes((MID, 2 * DH)), tile[EDGE:], tile[:MID]).astype(BF)
        out_ref[3 * g + 1, at : at + MID] = middle
        out_ref[3 * g + 1, at + MID : at + HALF] = jnp.zeros((HALF - MID, 2 * DH), BF)
        out_ref[3 * g + 2, at : at + HALF] = jnp.where(low, turn[MID : MID + HALF], tile[MID + HALF :]).astype(BF)


def pack_second(counts_ref, stagger_ref, keys_ref, values_ref, rates_ref, queries_ref, out_ref):
    scaled = scaled_values(values_ref[1], rates_ref, counts_ref, stagger_ref, 1)
    keys = keys_ref[1]
    out_ref[3 * PAIRS :, :EDGE] = jnp.zeros((NTOK - 3 * PAIRS, EDGE, 2 * DH), BF)
    for g in range(PAIRS):
        out_ref[3 * g + 1, 2 * MID : EDGE] = jnp.zeros((EDGE - 2 * MID, 2 * DH), BF)
        lanes = slice(2 * DH * g, 2 * DH * (g + 1))
        scatter_rows(out_ref, g, *pair_up(keys[:, lanes], scaled[:, lanes]))
    pack_queries(queries_ref[0], out_ref, EDGE)


def pack_third(queries_ref, out_ref):
    pack_queries(queries_ref[1], out_ref, 0)


def whole_weights(role_ref, rows_hbm, out_ref, counts_ref, rows_ref, sem):
    copy = pltpu.make_async_copy(rows_hbm.at[:, pl.ds(2 * MID, 2 * SHARE)], rows_ref, sem)
    copy.start()
    role = role_ref[0]
    copy.wait()
    for slot in range(2):
        start = pl.multiple_of(jnp.where(role == 1, slot * SHARE, EDGE - 2 * MID), SUB)
        gu = jnp.concatenate([rows_ref[s, pl.ds(start, UNITS)] for s in range(NTOK)], axis=0)
        w = jnp.concatenate([rows_ref[s, pl.ds(start + UNITS, UNITS)] for s in range(NTOK)], axis=0)
        gu = gu.astype(F32).T.astype(BF)
        w = w.astype(F32).T
        out_ref[slot] = jnp.concatenate([gu[:DH], gu[DH:], w[DH:].astype(BF)], axis=1)
        counts_ref[slot : slot + 1] = w[0:1].astype(jnp.int32)


def gradient(tick):
    def kernel(
        role_ref, counts_ref, stagger_ref, rows_hbm, weights_ref, own_ref, up_ref, down_ref,
        stack, acc, packed, steps, total_ref, rows_ref, sem,
    ):
        copy = pltpu.make_async_copy(rows_hbm.at[:, pl.ds(0, EDGE)], rows_ref, sem)
        copy.start()
        role, pair = role_ref[0], role_ref[1]
        zero = jnp.zeros((DH, FH), BF)

        def step(base, tile):
            kv = packed[pl.ds(pl.multiple_of(base, SUB), tile)]
            turn = kv.T
            k_t, v_t = turn[:DH], turn[DH:]
            piece = min(PIECE, tile)
            for f in range(0, FH, WIDTH):
                for m in range(0, tile, piece):
                    x = kv[m : m + piece]
                    half_gate = jnp.dot(x, stack[:, f : f + WIDTH], preferred_element_type=F32)
                    up = jnp.dot(x, stack[:, FH + f : FH + f + WIDTH], preferred_element_type=F32)
                    back = jnp.dot(x, stack[:, 2 * FH + f : 2 * FH + f + WIDTH], preferred_element_type=F32)
                    twice = jnp.tanh(half_gate) + 1.0
                    act = half_gate * twice
                    sig = 0.5 * twice
                    slope = sig + act * (1.0 - sig)
                    at = slice(m, m + piece)
                    steps[at, f : f + WIDTH] = (back * up * slope).astype(BF)
                    steps[at, FH + f : FH + f + WIDTH] = (back * act).astype(BF)
                    steps[at, 2 * FH + f : 2 * FH + f + WIDTH] = (act * up).astype(BF)
            for f in range(0, 3 * FH, WIDTH):
                left = k_t if f < 2 * FH else v_t
                acc[:, f : f + WIDTH] += jnp.dot(left, steps[:tile, f : f + WIDTH], preferred_element_type=F32)

        def head(slot, begin, place, blocks):
            w = weights_ref[slot]
            half = (w[:, :FH].astype(F32) * 0.5).astype(BF)
            stack[:DH] = jnp.concatenate([half, w[:, FH : 2 * FH], zero], axis=1)
            stack[DH:] = jnp.concatenate([zero, zero, w[:, 2 * FH :]], axis=1)
            acc[...] = jnp.zeros((DH, 3 * FH), F32)
            start = stagger_ref[2 * pair + slot]
            lead = start // SUB

            def from_shard(s, n):
                limit = counts_ref[slot, s * UNITS + tick * (UNITS // 2)]
                last = (start + limit - 1) // SUB
                used = ((2 << (last - lead)) - 1) << lead
                used = ((used | (used >> (ROWS // SUB))) >> (place // SUB)) * SUB
                for j in range(blocks):
                    packed[pl.ds(pl.multiple_of(n, SUB), SUB)] = rows_ref[s, pl.ds(begin + j * SUB, SUB)]
                    n = n + ((used >> j) & SUB)
                return n

            count = lax.fori_loop(0, NTOK, from_shard, jnp.int32(0))
            packed[pl.ds(pl.multiple_of(count, SUB), TILE)] = jnp.zeros((TILE, 2 * DH), BF)
            total_ref[0] = count

        def run(slot):
            count = total_ref[0]
            whole = count // TILE
            rest = count - whole * TILE
            whole = whole + jnp.where(rest > TILE // 2, 1, 0)

            def one(i, c):
                step(i * TILE, TILE)
                return c

            lax.fori_loop(0, whole, one, 0)

            @pl.when((rest > 0) & (rest <= TILE // 2))
            def _():
                step(whole * TILE, TILE // 2)

            own_ref[slot] = acc[...].astype(BF)

        copy.wait()

        def both(slot, c):
            @pl.when(role == 1)
            def _():
                head(slot, pl.multiple_of(slot * MID, SUB), jnp.where(slot == 0, EDGE, 0), MID // SUB)

            @pl.when(role != 1)
            def _():
                head(slot, 0, jnp.where(slot == 0, 0, MID), EDGE // SUB)

            run(slot)
            return c

        lax.fori_loop(jnp.where(role == 2, 1, 0), jnp.where(role == 0, 1, jnp.where(role == 3, 0, 2)), both, 0)
        up_ref[...] = own_ref[jnp.where(role == 0, 0, 1)]
        down_ref[...] = own_ref[jnp.where(role == 1, 0, 1)]

    return kernel


def renew(role_ref, weights_ref, own_ref, below_ref, above_ref, out_ref):
    role = role_ref[0]
    below, above = below_ref[...].astype(F32), above_ref[...].astype(F32)
    others = (jnp.where(role == 0, above, below), jnp.where(role == 1, above, below))
    for slot in range(2):
        base = weights_ref[slot].astype(F32)
        moved = base + (own_ref[slot].astype(F32) + others[slot])
        before = jnp.sum(base * base, axis=0, keepdims=True) + EPS
        after = jnp.sum(moved * moved, axis=0, keepdims=True) + EPS
        out_ref[slot] = (moved * (jnp.sqrt(before) / jnp.sqrt(after))).astype(BF)


def respond(tick):
    def kernel(role_ref, rows_hbm, weights_ref, *refs):
        if tick == 0:
            prev_hbm, (out_ref, stack, down, packed, hidden, loads) = None, refs
        else:
            prev_hbm, out_ref, stack, down, packed, hidden, loads = refs
        role = role_ref[0]
        first = EDGE if tick == 0 else 0
        copies = []
        for s in range(NTOK):
            target = packed.at[pl.ds(s * HALF, HALF)]
            copies.append(pltpu.make_async_copy(rows_hbm.at[s, pl.ds(first, HALF)], target, loads.at[s]))
            copies[-1].start()
        if tick == 1:
            earlier = pltpu.make_async_copy(prev_hbm, out_ref.at[:, pl.ds(0, HALF)], loads.at[NTOK])
            earlier.start()
        nothing = jnp.zeros((DH, FH), F32)
        for side in range(2):
            w = weights_ref[jnp.where(role == 2, 1, jnp.where(role == 1, side, 0))]
            half = (w[:, :FH].astype(F32) * 0.5).astype(BF)
            mine = jnp.concatenate([half, w[:, FH : 2 * FH]], axis=1)
            stack[side, side * DH : (side + 1) * DH] = mine
            stack[side, (1 - side) * DH : (2 - side) * DH] = jnp.zeros((DH, 2 * FH), BF)
            back = w[:, 2 * FH :].astype(F32)
            turn = jnp.concatenate([back, nothing] if side == 0 else [nothing, back], axis=0).T.astype(BF)
            down[side * FH : (side + 1) * FH] = turn
        for copy in copies:
            copy.wait()

        def step(i, c):
            tile = pl.ds(pl.multiple_of(i * PIECE, PIECE), PIECE)
            q = packed[tile]
            for side in range(2):
                for f in range(0, FH, WIDTH):
                    half_gate = jnp.dot(q, stack[side, :, f : f + WIDTH], preferred_element_type=F32)
                    up = jnp.dot(q, stack[side, :, FH + f : FH + f + WIDTH], preferred_element_type=F32)
                    value = half_gate * (jnp.tanh(half_gate) + 1.0) * up
                    hidden[:, side * FH + f : side * FH + f + WIDTH] = value.astype(BF)
            packed[tile] = jnp.dot(hidden[...], down[...], preferred_element_type=F32).astype(BF)
            return c

        lax.fori_loop(0, NTOK * HALF // PIECE, step, 0)
        at = tick * HALF
        for s in range(NTOK):
            out_ref[s, at : at + HALF] = packed[s * HALF : (s + 1) * HALF]
        if tick == 1:
            w = jnp.where(role == 0, weights_ref[0].astype(F32), weights_ref[1].astype(F32))
            gu = jnp.concatenate([w[:, :FH], w[:, FH : 2 * FH]], axis=0).T.astype(BF)
            dn = jnp.concatenate([w[:, 2 * FH :], nothing], axis=0).T.astype(BF)
            for s in range(NTOK):
                out_ref[s, 2 * HALF : 2 * HALF + UNITS] = gu[s * UNITS : (s + 1) * UNITS]
                out_ref[s, 2 * HALF + UNITS :] = dn[s * UNITS : (s + 1) * UNITS]
            earlier.wait()

    return kernel


def unpack(rows_ref, answers_ref, gate_ref, up_ref, down_ref):
    for g in range(PAIRS):
        lanes = slice(2 * DH * g, 2 * DH * (g + 1))
        for t in range(2):
            one, mid, two = (rows_ref[3 * g + d, t * HALF : (t + 1) * HALF].astype(F32) for d in range(3))
            first = jnp.concatenate([one, pltpu.roll(one, DH, 1), mid[:MID]], axis=0)
            second = jnp.concatenate([mid[:MID], pltpu.roll(two, DH, 1), two], axis=0)
            answers_ref[t, :, lanes] = jnp.where(low_lanes(first.shape), first, second).astype(BF)
        for h in range(2):
            share = rows_ref[3 * g + 2 * h, 2 * HALF :]
            gate_ref[2 * g + h] = share[:UNITS, :DH]
            up_ref[2 * g + h] = swap(share[:UNITS])[:, :DH]
            down_ref[2 * g + h] = share[UNITS:, :DH]


def call(kernel, outs, args, scalars=0, scratch=(), remote=(), far=False):
    places = [pltpu.SMEM if n < scalars else pltpu.HBM if n in remote else pltpu.VMEM for n in range(len(args))]
    args = [pltpu.with_memory_space_constraint(a, p) if p == pltpu.HBM else a for a, p in zip(args, places)]
    many = isinstance(outs, (tuple, list))
    out = lambda: pl.BlockSpec(memory_space=pltpu.HBM if far else pltpu.VMEM)
    if far:
        outs = pltpu.HBM(outs.shape, outs.dtype)
    return pl.pallas_call(
        kernel,
        out_shape=outs,
        in_specs=[pl.BlockSpec(memory_space=p) for p in places],
        out_specs=tuple(out() for _ in outs) if many else out(),
        scratch_shapes=list(scratch),
        compiler_params=pltpu.CompilerParams(vmem_limit_bytes=24 * 1024 * 1024),
    )(*args)


def shape(*dims):
    return jax.ShapeDtypeStruct(dims, BF)


def exchange(rows):
    result = lax.all_to_all(rows.reshape(-1, 2 * DH), "tok", split_axis=0, concat_axis=0, tiled=True)
    return result.reshape(rows.shape)


def program(keys, values, queries, rates, counts, stagger, gate_in, up_in, down_in, entry_gate, entry_up, entry_down):
    me = lax.axis_index("tok")
    pair = jnp.minimum(me // 3, PAIRS - 1)
    role = jnp.stack([jnp.where(me < 3 * PAIRS, me % 3, 3), pair]).astype(jnp.int32)
    keys, values, queries = keys[0], values[0], queries[0]
    rates = jnp.transpose(rates[0], (2, 0, 1))
    counts = counts[0, :, 0]
    shares = [jnp.transpose(w[0], (0, 2, 1)) for w in (gate_in, up_in, down_in)]
    tokens = (counts, stagger, keys, values, rates)
    scratch = [pltpu.VMEM((ROWS, HEADS * DH), BF)] * 2 + [pltpu.VMEM(rates.shape, BF)]
    scratch += [pltpu.VMEM((HEADS, UNITS, DH), BF)] * 3 + [pltpu.VMEM((NTOK, IN_ROWS, 2 * DH), BF)]
    scratch += [pltpu.SemaphoreType.DMA((6,)), pltpu.SemaphoreType.DMA((PAIRS + 1,))]
    operands = (*tokens, *shares)
    packed0 = call(pack_first, shape(NTOK, IN_ROWS, 2 * DH), operands, 2, scratch, range(2, len(operands)), True)
    rows0 = exchange(packed0)
    tokens, queries, packed0 = lax.optimization_barrier((tokens, queries, packed0))
    packed1 = call(pack_second, shape(NTOK, EDGE + HALF, 2 * DH), (*tokens, queries), 2)
    packed_q = call(pack_third, shape(NTOK, HALF, 2 * DH), (queries,))
    rows0, packed1, packed_q = lax.optimization_barrier((rows0, packed1, packed_q))
    rows1 = exchange(packed1)
    entries = jnp.concatenate(
        [lax.dynamic_slice_in_dim(e, 2 * pair, 2, 0) for e in (entry_gate, entry_up, entry_down)], axis=2
    )

    weight = shape(DH, 3 * FH)
    weights = shape(2, DH, 3 * FH)
    stacked = (pltpu.VMEM((2 * DH, 3 * FH), BF), pltpu.VMEM((DH, 3 * FH), F32))
    scratch = (*stacked, pltpu.VMEM((PACKED, 2 * DH), BF), pltpu.VMEM((TILE, 3 * FH), BF), pltpu.SMEM((1,), jnp.int32))
    scratch += (pltpu.VMEM((NTOK, EDGE, 2 * DH), BF), pltpu.SemaphoreType.DMA)

    def advance(tick, rows, current, limits):
        own, up, down = call(
            gradient(tick), (weights, weight, weight), (role, limits, stagger, rows, current), 3, scratch, (3,)
        )
        below = lax.ppermute(up, "tok", UPS)
        above = lax.ppermute(down, "tok", DOWNS)
        return call(renew, weights, (role, current, own, below, above), 1)

    current, limits = call(
        whole_weights,
        (weights, jax.ShapeDtypeStruct((2, FH), jnp.int32)),
        (role, rows0),
        1,
        (pltpu.VMEM((NTOK, 2 * SHARE, 2 * DH), BF), pltpu.SemaphoreType.DMA),
        (1,),
    )
    first = advance(0, rows0, current, limits)
    first, packed_q = lax.optimization_barrier((first, packed_q))
    rows_q = exchange(packed_q)
    size = lax.axis_size("block")
    passed = lax.ppermute(first, "block", [(b, b + 1) for b in range(size - 1)])
    second = advance(1, rows1, jnp.where(lax.axis_index("block") == 0, entries, passed), limits)

    scratch_q = (
        pltpu.VMEM((2, 2 * DH, 2 * FH), BF),
        pltpu.VMEM((2 * FH, 2 * DH), BF),
        pltpu.VMEM((NTOK * HALF, 2 * DH), BF),
        pltpu.VMEM((PIECE, 2 * FH), BF),
        pltpu.SemaphoreType.DMA((NTOK + 1,)),
    )
    answers0 = call(respond(0), shape(NTOK, HALF, 2 * DH), (role, rows1, first), 1, scratch_q, (1,))
    operands = (role, rows_q, second, answers0)
    packed = call(respond(1), shape(NTOK, OUT_ROWS, 2 * DH), operands, 1, scratch_q, (1, 3))
    answers, gate, up, down = call(
        unpack, (shape(2, ROWS, HEADS * DH),) + (shape(HEADS, UNITS, DH),) * 3, (exchange(packed),)
    )
    return (answers[None], *(jnp.transpose(w, (0, 2, 1))[None] for w in (gate, up, down)))


def solution(mesh):
    tokens = P("block", None, "tok", None)
    share = P("block", None, None, "tok")
    return jax.shard_map(
        program,
        mesh=mesh,
        in_specs=(tokens,) * 5 + (P(),) + (share,) * 3 + (P(),) * 3,
        out_specs=(tokens, share, share, share),
        check_vma=False,
    )
```

```python
import jax
import jax.numpy as jnp
from jax import lax
from jax.experimental import pallas as pl
from jax.experimental.pallas import tpu as pltpu
from jax.sharding import PartitionSpec as P

EPS = 1e-06
BF = jnp.bfloat16
F32 = jnp.float32

HEADS = 20
DH = 64
FH = 512
ROWS = 256
NTOK = 32
UNITS = FH // NTOK
PAIRS = HEADS // 2
EDGE = 176
MID = ROWS - EDGE
SUB = 16
TILE = 512
PER = TILE // SUB
SHARE = 2 * UNITS
IN_ROWS = 224
MID_BLOCKS = (1, 4, 7, 10, 13)
EDGE_BLOCKS = tuple(b for b in range(ROWS // SUB) if b not in MID_BLOCKS)
HALF = EDGE // 2
OUT_ROWS = 2 * HALF + SHARE
WIDTH = 256
PIECE = 256
PACKED = NTOK * EDGE + TILE
UPS = [(3 * g + a, 3 * g + a + 1) for g in range(PAIRS) for a in (0, 1)]
DOWNS = [(3 * g + a + 1, 3 * g + a) for g in range(PAIRS) for a in (0, 1)]


def low_lanes(shape):
    return lax.broadcasted_iota(jnp.int32, shape, 1) < DH


def swap(x):
    return pltpu.roll(x.astype(F32), DH, 1).astype(x.dtype)


def pair_up(left, right):
    low = low_lanes(left.shape)
    return jnp.where(low, left, swap(right)), jnp.where(low, swap(left), right)


def scatter_rows(out_ref, g, first, second):
    for j, b in enumerate(EDGE_BLOCKS):
        to, of = slice(j * SUB, (j + 1) * SUB), slice(b * SUB, (b + 1) * SUB)
        out_ref[3 * g, to] = first[of]
        out_ref[3 * g + 2, to] = second[of]
    for j, b in enumerate(MID_BLOCKS):
        of = slice(b * SUB, (b + 1) * SUB)
        out_ref[3 * g + 1, j * SUB : (j + 1) * SUB] = first[of]
        out_ref[3 * g + 1, MID + j * SUB : MID + (j + 1) * SUB] = second[of]


def spread_of():
    owner = lax.broadcasted_iota(jnp.int32, (HEADS, HEADS * DH), 1) // DH
    return (owner == lax.broadcasted_iota(jnp.int32, (HEADS, HEADS * DH), 0)).astype(F32).astype(BF)


def scaled_values(values, rates_ref, counts_ref, stagger_ref, tick):
    offset = lax.broadcasted_iota(jnp.int32, (1, ROWS), 1)
    scale = []
    for h in range(HEADS):
        inside = (offset - stagger_ref[h] + ROWS) & (ROWS - 1)
        scale.append(jnp.where(inside < counts_ref[tick, h], rates_ref[h, tick : tick + 1].astype(F32), 0.0))
    scale = jnp.concatenate(scale, axis=0).astype(BF)
    wide = lax.dot_general(scale, spread_of(), (((0,), (0,)), ((), ())), preferred_element_type=F32)
    return (values.astype(F32) * wide).astype(BF)


def pack_first(
    counts_ref, stagger_ref, keys_hbm, values_hbm, rates_hbm, gate_hbm, up_hbm, down_hbm, out_hbm,
    keys_ref, values_ref, rates_ref, gate_ref, up_ref, down_ref, out_ref, loads, stores,
):
    pairs = (
        (rates_hbm, rates_ref),
        (values_hbm.at[0], values_ref),
        (keys_hbm.at[0], keys_ref),
        (gate_hbm, gate_ref),
        (up_hbm, up_ref),
        (down_hbm, down_ref),
    )
    copies = [pltpu.make_async_copy(src, dst, loads.at[n]) for n, (src, dst) in enumerate(pairs)]
    for copy in copies:
        copy.start()
    out_ref[3 * PAIRS :] = jnp.zeros((NTOK - 3 * PAIRS, IN_ROWS, 2 * DH), BF)
    for g in range(PAIRS):
        for d in (0, 2):
            out_ref[3 * g + d, EDGE + SHARE :] = jnp.zeros((IN_ROWS - EDGE - SHARE, 2 * DH), BF)
    for copy in copies:
        copy.wait()
    scaled = scaled_values(values_ref[...], rates_ref, counts_ref, stagger_ref, 0)

    def share(h):
        half = (UNITS // 2, DH)
        counts = [jnp.full(half, counts_ref[t, h].astype(F32), F32) for t in range(2)]
        gu = jnp.concatenate([gate_ref[h], up_ref[h]], axis=1)
        w = jnp.concatenate([jnp.concatenate(counts, axis=0).astype(BF), down_ref[h]], axis=1)
        return jnp.concatenate([gu, w], axis=0)

    sent = []
    for g in range(PAIRS + 1):
        lo, n = 3 * g, 3 if g < PAIRS else NTOK - 3 * PAIRS
        if g < PAIRS:
            lanes = slice(2 * DH * g, 2 * DH * (g + 1))
            first, second = pair_up(keys_ref[:, lanes], scaled[:, lanes])
            scatter_rows(out_ref, g, first, second)
            shares = share(2 * g), share(2 * g + 1)
            out_ref[3 * g, EDGE : EDGE + SHARE] = shares[0]
            out_ref[3 * g + 1, 2 * MID : 2 * MID + SHARE] = shares[0]
            out_ref[3 * g + 1, 2 * MID + SHARE : 2 * MID + 2 * SHARE] = shares[1]
            out_ref[3 * g + 2, EDGE : EDGE + SHARE] = shares[1]
        sent.append(pltpu.make_async_copy(out_ref.at[pl.ds(lo, n)], out_hbm.at[pl.ds(lo, n)], stores.at[g]))
        sent[-1].start()
    for copy in sent:
        copy.wait()


def pack_queries(queries, out_ref, at):
    out_ref[3 * PAIRS :, at : at + HALF] = jnp.zeros((NTOK - 3 * PAIRS, HALF, 2 * DH), BF)
    for g in range(PAIRS):
        tile = queries[:, 2 * DH * g : 2 * DH * (g + 1)].astype(F32)
        turn = pltpu.roll(tile, DH, 1)
        low = low_lanes((HALF, 2 * DH))
        out_ref[3 * g, at : at + HALF] = jnp.where(low, tile[:HALF], turn[HALF:EDGE]).astype(BF)
        middle = jnp.where(low_lanes((MID, 2 * DH)), tile[EDGE:], tile[:MID]).astype(BF)
        out_ref[3 * g + 1, at : at + MID] = middle
        out_ref[3 * g + 1, at + MID : at + HALF] = jnp.zeros((HALF - MID, 2 * DH), BF)
        out_ref[3 * g + 2, at : at + HALF] = jnp.where(low, turn[MID : MID + HALF], tile[MID + HALF :]).astype(BF)


def pack_second(counts_ref, stagger_ref, keys_ref, values_ref, rates_ref, queries_ref, out_ref):
    scaled = scaled_values(values_ref[1], rates_ref, counts_ref, stagger_ref, 1)
    keys = keys_ref[1]
    out_ref[3 * PAIRS :, :EDGE] = jnp.zeros((NTOK - 3 * PAIRS, EDGE, 2 * DH), BF)
    for g in range(PAIRS):
        out_ref[3 * g + 1, 2 * MID : EDGE] = jnp.zeros((EDGE - 2 * MID, 2 * DH), BF)
        lanes = slice(2 * DH * g, 2 * DH * (g + 1))
        scatter_rows(out_ref, g, *pair_up(keys[:, lanes], scaled[:, lanes]))
    for t in range(2):
        pack_queries(queries_ref[t], out_ref, EDGE + t * HALF)


def whole_weights(role_ref, rows_hbm, out_ref, counts_ref, rows_ref, sem):
    copy = pltpu.make_async_copy(rows_hbm.at[:, pl.ds(2 * MID, 2 * SHARE)], rows_ref, sem)
    copy.start()
    role = role_ref[0]
    copy.wait()
    for slot in range(2):
        start = pl.multiple_of(jnp.where(role == 1, slot * SHARE, EDGE - 2 * MID), SUB)
        gu = jnp.concatenate([rows_ref[s, pl.ds(start, UNITS)] for s in range(NTOK)], axis=0)
        w = jnp.concatenate([rows_ref[s, pl.ds(start + UNITS, UNITS)] for s in range(NTOK)], axis=0)
        gu = gu.astype(F32).T.astype(BF)
        w = w.astype(F32).T
        out_ref[slot] = jnp.concatenate([gu[:DH], gu[DH:], w[DH:].astype(BF)], axis=1)
        counts_ref[slot : slot + 1] = w[0:1].astype(jnp.int32)


def gradient(tick):
    def kernel(
        role_ref, counts_ref, stagger_ref, rows_hbm, weights_ref, own_ref, up_ref, down_ref,
        stack, acc, packed, steps, total_ref, rows_ref, sem,
    ):
        copy = pltpu.make_async_copy(rows_hbm.at[:, pl.ds(0, EDGE)], rows_ref, sem)
        copy.start()
        role, pair = role_ref[0], role_ref[1]
        zero = jnp.zeros((DH, FH), BF)

        def step(base, tile):
            kv = packed[pl.ds(pl.multiple_of(base, SUB), tile)]
            turn = kv.T
            k_t, v_t = turn[:DH], turn[DH:]
            piece = min(PIECE, tile)
            for f in range(0, FH, WIDTH):
                for m in range(0, tile, piece):
                    x = kv[m : m + piece]
                    half_gate = jnp.dot(x, stack[:, f : f + WIDTH], preferred_element_type=F32)
                    up = jnp.dot(x, stack[:, FH + f : FH + f + WIDTH], preferred_element_type=F32)
                    back = jnp.dot(x, stack[:, 2 * FH + f : 2 * FH + f + WIDTH], preferred_element_type=F32)
                    twice = jnp.tanh(half_gate) + 1.0
                    act = half_gate * twice
                    sig = 0.5 * twice
                    slope = sig + act * (1.0 - sig)
                    at = slice(m, m + piece)
                    steps[at, f : f + WIDTH] = (back * up * slope).astype(BF)
                    steps[at, FH + f : FH + f + WIDTH] = (back * act).astype(BF)
                    steps[at, 2 * FH + f : 2 * FH + f + WIDTH] = (act * up).astype(BF)
            for f in range(0, 3 * FH, WIDTH):
                left = k_t if f < 2 * FH else v_t
                acc[:, f : f + WIDTH] += jnp.dot(left, steps[:tile, f : f + WIDTH], preferred_element_type=F32)

        def head(slot, begin, blocks):
            w = weights_ref[slot]
            half = (w[:, :FH].astype(F32) * 0.5).astype(BF)
            stack[:DH] = jnp.concatenate([half, w[:, FH : 2 * FH], zero], axis=1)
            stack[DH:] = jnp.concatenate([zero, zero, w[:, 2 * FH :]], axis=1)
            acc[...] = jnp.zeros((DH, 3 * FH), F32)
            start = stagger_ref[2 * pair + slot]
            lead = start // SUB

            def from_shard(s, n):
                limit = counts_ref[slot, s * UNITS + tick * (UNITS // 2)]
                last = (start + limit - 1) // SUB
                used = ((2 << (last - lead)) - 1) << lead
                used = used | (used >> (ROWS // SUB))
                for j, b in enumerate(blocks):
                    packed[pl.ds(pl.multiple_of(n, SUB), SUB)] = rows_ref[s, pl.ds(begin + j * SUB, SUB)]
                    n = n + ((used >> b) & 1) * SUB
                return n

            count = lax.fori_loop(0, NTOK, from_shard, jnp.int32(0))
            packed[pl.ds(pl.multiple_of(count, SUB), TILE)] = jnp.zeros((TILE, 2 * DH), BF)
            total_ref[0] = count

        def run(slot):
            count = total_ref[0]
            whole = count // TILE
            rest = count - whole * TILE
            whole = whole + jnp.where(rest > TILE // 2, 1, 0)

            def one(i, c):
                step(i * TILE, TILE)
                return c

            lax.fori_loop(0, whole, one, 0)

            @pl.when((rest > 0) & (rest <= TILE // 2))
            def _():
                step(whole * TILE, TILE // 2)

            own_ref[slot] = acc[...].astype(BF)

        copy.wait()

        def both(slot, c):
            @pl.when(role == 1)
            def _():
                head(slot, pl.multiple_of(slot * MID, SUB), MID_BLOCKS)

            @pl.when(role != 1)
            def _():
                head(slot, 0, EDGE_BLOCKS)

            run(slot)
            return c

        lax.fori_loop(jnp.where(role == 2, 1, 0), jnp.where(role == 0, 1, jnp.where(role == 3, 0, 2)), both, 0)
        up_ref[...] = own_ref[jnp.where(role == 0, 0, 1)]
        down_ref[...] = own_ref[jnp.where(role == 1, 0, 1)]

    return kernel


def renew(role_ref, weights_ref, own_ref, below_ref, above_ref, out_ref):
    role = role_ref[0]
    below, above = below_ref[...].astype(F32), above_ref[...].astype(F32)
    others = (jnp.where(role == 0, above, below), jnp.where(role == 1, above, below))
    for slot in range(2):
        base = weights_ref[slot].astype(F32)
        moved = base + (own_ref[slot].astype(F32) + others[slot])
        before = jnp.sum(base * base, axis=0, keepdims=True) + EPS
        after = jnp.sum(moved * moved, axis=0, keepdims=True) + EPS
        out_ref[slot] = (moved * (jnp.sqrt(before) / jnp.sqrt(after))).astype(BF)


def respond(tick):
    def kernel(role_ref, rows_hbm, weights_ref, *refs):
        if tick == 0:
            prev_ref, (out_ref, stack, down, packed, hidden, loads) = None, refs
        else:
            prev_ref, out_ref, stack, down, packed, hidden, loads = refs
        role = role_ref[0]
        first = EDGE + tick * HALF
        copies = []
        for s in range(NTOK):
            target = packed.at[pl.ds(s * HALF, HALF)]
            copies.append(pltpu.make_async_copy(rows_hbm.at[s, pl.ds(first, HALF)], target, loads.at[s]))
            copies[-1].start()
        nothing = jnp.zeros((DH, FH), F32)
        for side in range(2):
            w = weights_ref[jnp.where(role == 2, 1, jnp.where(role == 1, side, 0))]
            half = (w[:, :FH].astype(F32) * 0.5).astype(BF)
            mine = jnp.concatenate([half, w[:, FH : 2 * FH]], axis=1)
            stack[side, side * DH : (side + 1) * DH] = mine
            stack[side, (1 - side) * DH : (2 - side) * DH] = jnp.zeros((DH, 2 * FH), BF)
            back = w[:, 2 * FH :].astype(F32)
            turn = jnp.concatenate([back, nothing] if side == 0 else [nothing, back], axis=0).T.astype(BF)
            down[side * FH : (side + 1) * FH] = turn
        for copy in copies:
            copy.wait()

        def step(i, c):
            tile = pl.ds(pl.multiple_of(i * PIECE, PIECE), PIECE)
            q = packed[tile]
            for side in range(2):
                for f in range(0, FH, WIDTH):
                    half_gate = jnp.dot(q, stack[side, :, f : f + WIDTH], preferred_element_type=F32)
                    up = jnp.dot(q, stack[side, :, FH + f : FH + f + WIDTH], preferred_element_type=F32)
                    value = half_gate * (jnp.tanh(half_gate) + 1.0) * up
                    hidden[:, side * FH + f : side * FH + f + WIDTH] = value.astype(BF)
            packed[tile] = jnp.dot(hidden[...], down[...], preferred_element_type=F32).astype(BF)
            return c

        lax.fori_loop(0, NTOK * HALF // PIECE, step, 0)
        at = tick * HALF
        for s in range(NTOK):
            out_ref[s, at : at + HALF] = packed[s * HALF : (s + 1) * HALF]
        if tick == 1:
            w = jnp.where(role == 0, weights_ref[0].astype(F32), weights_ref[1].astype(F32))
            gu = jnp.concatenate([w[:, :FH], w[:, FH : 2 * FH]], axis=0).T.astype(BF)
            dn = jnp.concatenate([w[:, 2 * FH :], nothing], axis=0).T.astype(BF)
            for s in range(NTOK):
                out_ref[s, :HALF] = prev_ref[s]
                out_ref[s, 2 * HALF : 2 * HALF + UNITS] = gu[s * UNITS : (s + 1) * UNITS]
                out_ref[s, 2 * HALF + UNITS :] = dn[s * UNITS : (s + 1) * UNITS]

    return kernel


def unpack(rows_ref, answers_ref, gate_ref, up_ref, down_ref):
    for g in range(PAIRS):
        lanes = slice(2 * DH * g, 2 * DH * (g + 1))
        for t in range(2):
            one, mid, two = (rows_ref[3 * g + d, t * HALF : (t + 1) * HALF].astype(F32) for d in range(3))
            first = jnp.concatenate([one, pltpu.roll(one, DH, 1), mid[:MID]], axis=0)
            second = jnp.concatenate([mid[:MID], pltpu.roll(two, DH, 1), two], axis=0)
            answers_ref[t, :, lanes] = jnp.where(low_lanes(first.shape), first, second).astype(BF)
        for h in range(2):
            share = rows_ref[3 * g + 2 * h, 2 * HALF :]
            gate_ref[2 * g + h] = share[:UNITS, :DH]
            up_ref[2 * g + h] = swap(share[:UNITS])[:, :DH]
            down_ref[2 * g + h] = share[UNITS:, :DH]


def call(kernel, name, outs, args, scalars=0, scratch=(), remote=(), far=False):
    places = [pltpu.SMEM if n < scalars else pltpu.HBM if n in remote else pltpu.VMEM for n in range(len(args))]
    args = [pltpu.with_memory_space_constraint(a, p) if p == pltpu.HBM else a for a, p in zip(args, places)]
    many = isinstance(outs, (tuple, list))
    out = lambda: pl.BlockSpec(memory_space=pltpu.HBM if far else pltpu.VMEM)
    if far:
        outs = pltpu.HBM(outs.shape, outs.dtype)
    return pl.pallas_call(
        kernel,
        name=name,
        out_shape=outs,
        in_specs=[pl.BlockSpec(memory_space=p) for p in places],
        out_specs=tuple(out() for _ in outs) if many else out(),
        scratch_shapes=list(scratch),
        compiler_params=pltpu.CompilerParams(vmem_limit_bytes=24 * 1024 * 1024),
    )(*args)


def shape(*dims):
    return jax.ShapeDtypeStruct(dims, BF)


def exchange(rows):
    result = lax.all_to_all(rows.reshape(-1, 2 * DH), "tok", split_axis=0, concat_axis=0, tiled=True)
    return result.reshape(rows.shape)


def shards(keys, values, queries, rates, counts, stagger, gate_in, up_in, down_in, entry_gate, entry_up, entry_down):
    me = lax.axis_index("tok")
    pair = jnp.minimum(me // 3, PAIRS - 1)
    role = jnp.stack([jnp.where(me < 3 * PAIRS, me % 3, 3), pair]).astype(jnp.int32)
    keys, values, queries = keys[0], values[0], queries[0]
    rates = jnp.transpose(rates[0], (2, 0, 1))
    counts = counts[0, :, 0]
    shares = [jnp.transpose(w[0], (0, 2, 1)) for w in (gate_in, up_in, down_in)]
    tokens = (counts, stagger, keys, values, rates)
    scratch = [pltpu.VMEM((ROWS, HEADS * DH), BF)] * 2 + [pltpu.VMEM(rates.shape, BF)]
    scratch += [pltpu.VMEM((HEADS, UNITS, DH), BF)] * 3 + [pltpu.VMEM((NTOK, IN_ROWS, 2 * DH), BF)]
    scratch += [pltpu.SemaphoreType.DMA((6,)), pltpu.SemaphoreType.DMA((PAIRS + 1,))]
    operands = (*tokens, *shares)
    packed0 = call(
        pack_first, "pack_first", shape(NTOK, IN_ROWS, 2 * DH), operands, 2, scratch, range(2, len(operands)), True
    )
    rows0 = exchange(packed0)
    tokens, queries, packed0 = lax.optimization_barrier((tokens, queries, packed0))
    packed1 = call(pack_second, "pack_second", shape(NTOK, EDGE + 2 * HALF, 2 * DH), (*tokens, queries), 2)
    rows0, packed1 = lax.optimization_barrier((rows0, packed1))
    rows1 = exchange(packed1)
    entries = jnp.concatenate(
        [lax.dynamic_slice_in_dim(e, 2 * pair, 2, 0) for e in (entry_gate, entry_up, entry_down)], axis=2
    )

    weight = shape(DH, 3 * FH)
    weights = shape(2, DH, 3 * FH)
    stacked = (pltpu.VMEM((2 * DH, 3 * FH), BF), pltpu.VMEM((DH, 3 * FH), F32))
    scratch = (*stacked, pltpu.VMEM((PACKED, 2 * DH), BF), pltpu.VMEM((TILE, 3 * FH), BF), pltpu.SMEM((1,), jnp.int32))
    scratch += (pltpu.VMEM((NTOK, EDGE, 2 * DH), BF), pltpu.SemaphoreType.DMA)

    def advance(tick, rows, current, limits):
        own, up, down = call(
            gradient(tick),
            "gradient",
            (weights, weight, weight),
            (role, limits, stagger, rows, current),
            3,
            scratch,
            (3,),
        )
        below = lax.ppermute(up, "tok", UPS)
        above = lax.ppermute(down, "tok", DOWNS)
        return call(renew, "renew", weights, (role, current, own, below, above), 1)

    current, limits = call(
        whole_weights,
        "whole_weights",
        (weights, jax.ShapeDtypeStruct((2, FH), jnp.int32)),
        (role, rows0),
        1,
        (pltpu.VMEM((NTOK, 2 * SHARE, 2 * DH), BF), pltpu.SemaphoreType.DMA),
        (1,),
    )
    first = advance(0, rows0, current, limits)
    size = lax.axis_size("block")
    passed = lax.ppermute(first, "block", [(b, b + 1) for b in range(size - 1)])
    second = advance(1, rows1, jnp.where(lax.axis_index("block") == 0, entries, passed), limits)

    scratch_q = (
        pltpu.VMEM((2, 2 * DH, 2 * FH), BF),
        pltpu.VMEM((2 * FH, 2 * DH), BF),
        pltpu.VMEM((NTOK * HALF, 2 * DH), BF),
        pltpu.VMEM((PIECE, 2 * FH), BF),
        pltpu.SemaphoreType.DMA((NTOK,)),
    )
    answers0 = call(respond(0), "respond_first", shape(NTOK, HALF, 2 * DH), (role, rows1, first), 1, scratch_q, (1,))
    operands = (role, rows1, second, answers0)
    packed = call(
        respond(1), "respond_second", shape(NTOK, OUT_ROWS, 2 * DH), operands, 1, scratch_q, (1,)
    )
    answers, gate, up, down = call(
        unpack,
        "unpack",
        (shape(2, ROWS, HEADS * DH),) + (shape(HEADS, UNITS, DH),) * 3,
        (exchange(packed),),
    )
    return (answers[None], *(jnp.transpose(w, (0, 2, 1))[None] for w in (gate, up, down)))


def solution(mesh):
    tokens = P("block", None, "tok", None)
    share = P("block", None, None, "tok")
    return jax.shard_map(
        shards,
        mesh=mesh,
        in_specs=(tokens,) * 5 + (P(),) + (share,) * 3 + (P(),) * 3,
        out_specs=(tokens, share, share, share),
        check_vma=False,
    )
```

```python
import jax
import jax.numpy as jnp
from jax import lax
from jax.experimental import pallas as pl
from jax.experimental.pallas import tpu as pltpu
from jax.sharding import PartitionSpec as P


EPS = 1e-06
BF = jnp.bfloat16
F32 = jnp.float32

HEADS = 20
DH = 64
FH = 512
ROWS = 256
NTOK = 32
UNITS = FH // NTOK
PAIRS = HEADS // 2
EDGE = 176
MID = ROWS - EDGE
SUB = 16
TILE = 512
SHARE = 2 * UNITS
IN_ROWS = 224
MID_BLOCKS = (1, 4, 7, 10, 13)
EDGE_BLOCKS = tuple(b for b in range(ROWS // SUB) if b not in MID_BLOCKS)
HALF = EDGE // 2
OUT_ROWS = 2 * HALF + SHARE
WIDTH = 256
PIECE = 256
PACKED = NTOK * EDGE + TILE
UPS = [(3 * g + a, 3 * g + a + 1) for g in range(PAIRS) for a in (0, 1)]
DOWNS = [(3 * g + a + 1, 3 * g + a) for g in range(PAIRS) for a in (0, 1)]


def low_lanes(shape):
    return lax.broadcasted_iota(jnp.int32, shape, 1) < DH


def swap(x):
    return pltpu.roll(x.astype(F32), DH, 1).astype(x.dtype)


def pair_up(left, right):
    low = low_lanes(left.shape)
    return jnp.where(low, left, swap(right)), jnp.where(low, swap(left), right)


def scatter_rows(out_ref, g, first, second):
    for j, b in enumerate(EDGE_BLOCKS):
        to, of = slice(j * SUB, (j + 1) * SUB), slice(b * SUB, (b + 1) * SUB)
        out_ref[3 * g, to] = first[of]
        out_ref[3 * g + 2, to] = second[of]
    for j, b in enumerate(MID_BLOCKS):
        of = slice(b * SUB, (b + 1) * SUB)
        out_ref[3 * g + 1, j * SUB : (j + 1) * SUB] = first[of]
        out_ref[3 * g + 1, MID + j * SUB : MID + (j + 1) * SUB] = second[of]


def spread_of():
    owner = lax.broadcasted_iota(jnp.int32, (HEADS, HEADS * DH), 1) // DH
    return (owner == lax.broadcasted_iota(jnp.int32, (HEADS, HEADS * DH), 0)).astype(F32).astype(BF)


def scaled_values(values, rates_ref, counts_ref, stagger_ref, tick):
    offset = lax.broadcasted_iota(jnp.int32, (1, ROWS), 1)
    scale = []
    for h in range(HEADS):
        inside = (offset - stagger_ref[h] + ROWS) & (ROWS - 1)
        scale.append(jnp.where(inside < counts_ref[tick, h], rates_ref[h, tick : tick + 1].astype(F32), 0.0))
    scale = jnp.concatenate(scale, axis=0).astype(BF)
    wide = lax.dot_general(scale, spread_of(), (((0,), (0,)), ((), ())), preferred_element_type=F32)
    return (values.astype(F32) * wide).astype(BF)


def pack_first(
    counts_ref, stagger_ref, keys_hbm, values_hbm, rates_hbm, gate_hbm, up_hbm, down_hbm, out_hbm,
    keys_ref, values_ref, rates_ref, gate_ref, up_ref, down_ref, out_ref, loads, stores,
):
    pairs = (
        (rates_hbm, rates_ref),
        (values_hbm.at[0], values_ref),
        (keys_hbm.at[0], keys_ref),
        (gate_hbm, gate_ref),
        (up_hbm, up_ref),
        (down_hbm, down_ref),
    )
    copies = [pltpu.make_async_copy(src, dst, loads.at[n]) for n, (src, dst) in enumerate(pairs)]
    for copy in copies:
        copy.start()
    out_ref[3 * PAIRS :] = jnp.zeros((NTOK - 3 * PAIRS, IN_ROWS, 2 * DH), BF)
    for g in range(PAIRS):
        for d in (0, 2):
            out_ref[3 * g + d, EDGE + SHARE :] = jnp.zeros((IN_ROWS - EDGE - SHARE, 2 * DH), BF)
    for copy in copies:
        copy.wait()
    scaled = scaled_values(values_ref[...], rates_ref, counts_ref, stagger_ref, 0)

    def share(h):
        half = (UNITS // 2, DH)
        counts = [jnp.full(half, counts_ref[t, h].astype(F32), F32) for t in range(2)]
        gu = jnp.concatenate([gate_ref[h], up_ref[h]], axis=1)
        w = jnp.concatenate([jnp.concatenate(counts, axis=0).astype(BF), down_ref[h]], axis=1)
        return jnp.concatenate([gu, w], axis=0)

    sent = []
    for g in range(PAIRS + 1):
        lo, n = 3 * g, 3 if g < PAIRS else NTOK - 3 * PAIRS
        if g < PAIRS:
            lanes = slice(2 * DH * g, 2 * DH * (g + 1))
            first, second = pair_up(keys_ref[:, lanes], scaled[:, lanes])
            scatter_rows(out_ref, g, first, second)
            shares = share(2 * g), share(2 * g + 1)
            out_ref[3 * g, EDGE : EDGE + SHARE] = shares[0]
            out_ref[3 * g + 1, 2 * MID : 2 * MID + SHARE] = shares[0]
            out_ref[3 * g + 1, 2 * MID + SHARE : 2 * MID + 2 * SHARE] = shares[1]
            out_ref[3 * g + 2, EDGE : EDGE + SHARE] = shares[1]
        sent.append(pltpu.make_async_copy(out_ref.at[pl.ds(lo, n)], out_hbm.at[pl.ds(lo, n)], stores.at[g]))
        sent[-1].start()
    for copy in sent:
        copy.wait()


def pack_queries(queries, out_ref, at):
    out_ref[3 * PAIRS :, at : at + HALF] = jnp.zeros((NTOK - 3 * PAIRS, HALF, 2 * DH), BF)
    for g in range(PAIRS):
        tile = queries[:, 2 * DH * g : 2 * DH * (g + 1)].astype(F32)
        turn = pltpu.roll(tile, DH, 1)
        low = low_lanes((HALF, 2 * DH))
        out_ref[3 * g, at : at + HALF] = jnp.where(low, tile[:HALF], turn[HALF:EDGE]).astype(BF)
        middle = jnp.where(low_lanes((MID, 2 * DH)), tile[EDGE:], tile[:MID]).astype(BF)
        out_ref[3 * g + 1, at : at + MID] = middle
        out_ref[3 * g + 1, at + MID : at + HALF] = jnp.zeros((HALF - MID, 2 * DH), BF)
        out_ref[3 * g + 2, at : at + HALF] = jnp.where(low, turn[MID : MID + HALF], tile[MID + HALF :]).astype(BF)


def pack_second(counts_ref, stagger_ref, keys_ref, values_ref, rates_ref, queries_ref, out_ref):
    scaled = scaled_values(values_ref[1], rates_ref, counts_ref, stagger_ref, 1)
    keys = keys_ref[1]
    out_ref[3 * PAIRS :, :EDGE] = jnp.zeros((NTOK - 3 * PAIRS, EDGE, 2 * DH), BF)
    for g in range(PAIRS):
        out_ref[3 * g + 1, 2 * MID : EDGE] = jnp.zeros((EDGE - 2 * MID, 2 * DH), BF)
        lanes = slice(2 * DH * g, 2 * DH * (g + 1))
        scatter_rows(out_ref, g, *pair_up(keys[:, lanes], scaled[:, lanes]))
    pack_queries(queries_ref[0], out_ref, EDGE)


def pack_third(queries_ref, out_ref):
    pack_queries(queries_ref[1], out_ref, 0)


def whole_weights(role_ref, rows_hbm, out_ref, counts_ref, rows_ref, sem):
    copy = pltpu.make_async_copy(rows_hbm.at[:, pl.ds(2 * MID, 2 * SHARE)], rows_ref, sem)
    copy.start()
    role = role_ref[0]
    copy.wait()
    for slot in range(2):
        start = pl.multiple_of(jnp.where(role == 1, slot * SHARE, EDGE - 2 * MID), SUB)
        gu = jnp.concatenate([rows_ref[s, pl.ds(start, UNITS)] for s in range(NTOK)], axis=0)
        w = jnp.concatenate([rows_ref[s, pl.ds(start + UNITS, UNITS)] for s in range(NTOK)], axis=0)
        gu = gu.astype(F32).T.astype(BF)
        w = w.astype(F32).T
        out_ref[slot] = jnp.concatenate([gu[:DH], gu[DH:], w[DH:].astype(BF)], axis=1)
        counts_ref[slot : slot + 1] = w[0:1].astype(jnp.int32)


def gradient(tick):
    def kernel(
        role_ref, counts_ref, stagger_ref, rows_hbm, weights_ref, own_ref, up_ref, down_ref,
        stack, acc, packed, steps, total_ref, rows_ref, sem,
    ):
        copy = pltpu.make_async_copy(rows_hbm.at[:, pl.ds(0, EDGE)], rows_ref, sem)
        copy.start()
        role, pair = role_ref[0], role_ref[1]
        zero = jnp.zeros((DH, FH), BF)

        def step(base, tile):
            kv = packed[pl.ds(pl.multiple_of(base, SUB), tile)]
            turn = kv.T
            k_t, v_t = turn[:DH], turn[DH:]
            piece = min(PIECE, tile)
            for f in range(0, FH, WIDTH):
                for m in range(0, tile, piece):
                    x = kv[m : m + piece]
                    half_gate = jnp.dot(x, stack[:, f : f + WIDTH], preferred_element_type=F32)
                    up = jnp.dot(x, stack[:, FH + f : FH + f + WIDTH], preferred_element_type=F32)
                    back = jnp.dot(x, stack[:, 2 * FH + f : 2 * FH + f + WIDTH], preferred_element_type=F32)
                    twice = jnp.tanh(half_gate) + 1.0
                    act = half_gate * twice
                    sig = 0.5 * twice
                    slope = sig + act * (1.0 - sig)
                    at = slice(m, m + piece)
                    steps[at, f : f + WIDTH] = (back * up * slope).astype(BF)
                    steps[at, FH + f : FH + f + WIDTH] = (back * act).astype(BF)
                    steps[at, 2 * FH + f : 2 * FH + f + WIDTH] = (act * up).astype(BF)
            for f in range(0, 3 * FH, WIDTH):
                left = k_t if f < 2 * FH else v_t
                acc[:, f : f + WIDTH] += jnp.dot(left, steps[:tile, f : f + WIDTH], preferred_element_type=F32)

        def head(slot, begin, blocks):
            w = weights_ref[slot]
            half = (w[:, :FH].astype(F32) * 0.5).astype(BF)
            stack[:DH] = jnp.concatenate([half, w[:, FH : 2 * FH], zero], axis=1)
            stack[DH:] = jnp.concatenate([zero, zero, w[:, 2 * FH :]], axis=1)
            acc[...] = jnp.zeros((DH, 3 * FH), F32)
            start = stagger_ref[2 * pair + slot]
            lead = start // SUB

            def from_shard(s, n):
                limit = counts_ref[slot, s * UNITS + tick * (UNITS // 2)]
                last = (start + limit - 1) // SUB
                used = ((2 << (last - lead)) - 1) << lead
                used = used | (used >> (ROWS // SUB))
                for j, b in enumerate(blocks):
                    packed[pl.ds(pl.multiple_of(n, SUB), SUB)] = rows_ref[s, pl.ds(begin + j * SUB, SUB)]
                    n = n + ((used >> b) & 1) * SUB
                return n

            count = lax.fori_loop(0, NTOK, from_shard, jnp.int32(0))
            packed[pl.ds(pl.multiple_of(count, SUB), TILE)] = jnp.zeros((TILE, 2 * DH), BF)
            total_ref[0] = count

        def run(slot):
            count = total_ref[0]
            whole = count // TILE
            rest = count - whole * TILE
            whole = whole + jnp.where(rest > TILE // 2, 1, 0)

            def one(i, c):
                step(i * TILE, TILE)
                return c

            lax.fori_loop(0, whole, one, 0)

            @pl.when((rest > 0) & (rest <= TILE // 2))
            def _():
                step(whole * TILE, TILE // 2)

            own_ref[slot] = acc[...].astype(BF)

        copy.wait()

        def both(slot, c):
            @pl.when(role == 1)
            def _():
                head(slot, pl.multiple_of(slot * MID, SUB), MID_BLOCKS)

            @pl.when(role != 1)
            def _():
                head(slot, 0, EDGE_BLOCKS)

            run(slot)
            return c

        lax.fori_loop(jnp.where(role == 2, 1, 0), jnp.where(role == 0, 1, jnp.where(role == 3, 0, 2)), both, 0)
        up_ref[...] = own_ref[jnp.where(role == 0, 0, 1)]
        down_ref[...] = own_ref[jnp.where(role == 1, 0, 1)]

    return kernel


def renew(role_ref, weights_ref, own_ref, below_ref, above_ref, out_ref):
    role = role_ref[0]
    below, above = below_ref[...].astype(F32), above_ref[...].astype(F32)
    others = (jnp.where(role == 0, above, below), jnp.where(role == 1, above, below))
    for slot in range(2):
        base = weights_ref[slot].astype(F32)
        moved = base + (own_ref[slot].astype(F32) + others[slot])
        before = jnp.sum(base * base, axis=0, keepdims=True) + EPS
        after = jnp.sum(moved * moved, axis=0, keepdims=True) + EPS
        out_ref[slot] = (moved * (jnp.sqrt(before) / jnp.sqrt(after))).astype(BF)


def respond(tick):
    def kernel(role_ref, rows_ref, weights_ref, *refs):
        if tick == 0:
            prev_ref, (out_ref, stack, down, packed, hidden, loads) = None, refs
        else:
            prev_ref, out_ref, stack, down, packed, hidden, loads = refs
        role = role_ref[0]
        copies = []
        for s in range(NTOK):
            if tick == 1:
                packed[s * HALF : (s + 1) * HALF] = rows_ref[s]
                continue
            target = packed.at[pl.ds(s * HALF, HALF)]
            copies.append(pltpu.make_async_copy(rows_ref.at[s, pl.ds(EDGE, HALF)], target, loads.at[s]))
            copies[-1].start()
        nothing = jnp.zeros((DH, FH), F32)
        for side in range(2):
            w = weights_ref[jnp.where(role == 2, 1, jnp.where(role == 1, side, 0))]
            half = (w[:, :FH].astype(F32) * 0.5).astype(BF)
            mine = jnp.concatenate([half, w[:, FH : 2 * FH]], axis=1)
            stack[side, side * DH : (side + 1) * DH] = mine
            stack[side, (1 - side) * DH : (2 - side) * DH] = jnp.zeros((DH, 2 * FH), BF)
            back = w[:, 2 * FH :].astype(F32)
            turn = jnp.concatenate([back, nothing] if side == 0 else [nothing, back], axis=0).T.astype(BF)
            down[side * FH : (side + 1) * FH] = turn
        for copy in copies:
            copy.wait()

        def step(i, c):
            tile = pl.ds(pl.multiple_of(i * PIECE, PIECE), PIECE)
            q = packed[tile]
            for side in range(2):
                for f in range(0, FH, WIDTH):
                    half_gate = jnp.dot(q, stack[side, :, f : f + WIDTH], preferred_element_type=F32)
                    up = jnp.dot(q, stack[side, :, FH + f : FH + f + WIDTH], preferred_element_type=F32)
                    value = half_gate * (jnp.tanh(half_gate) + 1.0) * up
                    hidden[:, side * FH + f : side * FH + f + WIDTH] = value.astype(BF)
            packed[tile] = jnp.dot(hidden[...], down[...], preferred_element_type=F32).astype(BF)
            return c

        lax.fori_loop(0, NTOK * HALF // PIECE, step, 0)
        at = tick * HALF
        for s in range(NTOK):
            out_ref[s, at : at + HALF] = packed[s * HALF : (s + 1) * HALF]
        if tick == 1:
            w = jnp.where(role == 0, weights_ref[0].astype(F32), weights_ref[1].astype(F32))
            gu = jnp.concatenate([w[:, :FH], w[:, FH : 2 * FH]], axis=0).T.astype(BF)
            dn = jnp.concatenate([w[:, 2 * FH :], nothing], axis=0).T.astype(BF)
            for s in range(NTOK):
                out_ref[s, :HALF] = prev_ref[s]
                out_ref[s, 2 * HALF : 2 * HALF + UNITS] = gu[s * UNITS : (s + 1) * UNITS]
                out_ref[s, 2 * HALF + UNITS :] = dn[s * UNITS : (s + 1) * UNITS]

    return kernel


def unpack(rows_ref, answers_ref, gate_ref, up_ref, down_ref):
    for g in range(PAIRS):
        lanes = slice(2 * DH * g, 2 * DH * (g + 1))
        for t in range(2):
            one, mid, two = (rows_ref[3 * g + d, t * HALF : (t + 1) * HALF].astype(F32) for d in range(3))
            first = jnp.concatenate([one, pltpu.roll(one, DH, 1), mid[:MID]], axis=0)
            second = jnp.concatenate([mid[:MID], pltpu.roll(two, DH, 1), two], axis=0)
            answers_ref[t, :, lanes] = jnp.where(low_lanes(first.shape), first, second).astype(BF)
        for h in range(2):
            share = rows_ref[3 * g + 2 * h, 2 * HALF :]
            gate_ref[2 * g + h] = share[:UNITS, :DH]
            up_ref[2 * g + h] = swap(share[:UNITS])[:, :DH]
            down_ref[2 * g + h] = share[UNITS:, :DH]


def call(kernel, outs, args, scalars=0, scratch=(), remote=(), far=False):
    places = [pltpu.SMEM if n < scalars else pltpu.HBM if n in remote else pltpu.VMEM for n in range(len(args))]
    args = [pltpu.with_memory_space_constraint(a, p) if p == pltpu.HBM else a for a, p in zip(args, places)]
    many = isinstance(outs, (tuple, list))
    out = lambda: pl.BlockSpec(memory_space=pltpu.HBM if far else pltpu.VMEM)
    if far:
        outs = pltpu.HBM(outs.shape, outs.dtype)
    return pl.pallas_call(
        kernel,
        out_shape=outs,
        in_specs=[pl.BlockSpec(memory_space=p) for p in places],
        out_specs=tuple(out() for _ in outs) if many else out(),
        scratch_shapes=list(scratch),
        compiler_params=pltpu.CompilerParams(vmem_limit_bytes=24 * 1024 * 1024),
    )(*args)


def shape(*dims):
    return jax.ShapeDtypeStruct(dims, BF)


def exchange(rows):
    result = lax.all_to_all(rows.reshape(-1, 2 * DH), "tok", split_axis=0, concat_axis=0, tiled=True)
    return result.reshape(rows.shape)


def program(keys, values, queries, rates, counts, stagger, gate_in, up_in, down_in, entry_gate, entry_up, entry_down):
    me = lax.axis_index("tok")
    pair = jnp.minimum(me // 3, PAIRS - 1)
    role = jnp.stack([jnp.where(me < 3 * PAIRS, me % 3, 3), pair]).astype(jnp.int32)
    keys, values, queries = keys[0], values[0], queries[0]
    rates = jnp.transpose(rates[0], (2, 0, 1))
    counts = counts[0, :, 0]
    shares = [jnp.transpose(w[0], (0, 2, 1)) for w in (gate_in, up_in, down_in)]
    tokens = (counts, stagger, keys, values, rates)
    scratch = [pltpu.VMEM((ROWS, HEADS * DH), BF)] * 2 + [pltpu.VMEM(rates.shape, BF)]
    scratch += [pltpu.VMEM((HEADS, UNITS, DH), BF)] * 3 + [pltpu.VMEM((NTOK, IN_ROWS, 2 * DH), BF)]
    scratch += [pltpu.SemaphoreType.DMA((6,)), pltpu.SemaphoreType.DMA((PAIRS + 1,))]
    operands = (*tokens, *shares)
    packed0 = call(pack_first, shape(NTOK, IN_ROWS, 2 * DH), operands, 2, scratch, range(2, len(operands)), True)
    rows0 = exchange(packed0)
    tokens, queries, packed0 = lax.optimization_barrier((tokens, queries, packed0))
    packed1 = call(pack_second, shape(NTOK, EDGE + HALF, 2 * DH), (*tokens, queries), 2)
    packed_q = call(pack_third, shape(NTOK, HALF, 2 * DH), (queries,))
    rows0, packed1, packed_q = lax.optimization_barrier((rows0, packed1, packed_q))
    rows1 = exchange(packed1)
    entries = jnp.concatenate(
        [lax.dynamic_slice_in_dim(e, 2 * pair, 2, 0) for e in (entry_gate, entry_up, entry_down)], axis=2
    )

    weight = shape(DH, 3 * FH)
    weights = shape(2, DH, 3 * FH)
    stacked = (pltpu.VMEM((2 * DH, 3 * FH), BF), pltpu.VMEM((DH, 3 * FH), F32))
    scratch = (*stacked, pltpu.VMEM((PACKED, 2 * DH), BF), pltpu.VMEM((TILE, 3 * FH), BF), pltpu.SMEM((1,), jnp.int32))
    scratch += (pltpu.VMEM((NTOK, EDGE, 2 * DH), BF), pltpu.SemaphoreType.DMA)

    def advance(tick, rows, current, limits):
        own, up, down = call(
            gradient(tick), (weights, weight, weight), (role, limits, stagger, rows, current), 3, scratch, (3,)
        )
        below = lax.ppermute(up, "tok", UPS)
        above = lax.ppermute(down, "tok", DOWNS)
        return call(renew, weights, (role, current, own, below, above), 1)

    current, limits = call(
        whole_weights,
        (weights, jax.ShapeDtypeStruct((2, FH), jnp.int32)),
        (role, rows0),
        1,
        (pltpu.VMEM((NTOK, 2 * SHARE, 2 * DH), BF), pltpu.SemaphoreType.DMA),
        (1,),
    )
    first = advance(0, rows0, current, limits)
    first, packed_q = lax.optimization_barrier((first, packed_q))
    rows_q = exchange(packed_q)
    size = lax.axis_size("block")
    passed = lax.ppermute(first, "block", [(b, b + 1) for b in range(size - 1)])
    second = advance(1, rows1, jnp.where(lax.axis_index("block") == 0, entries, passed), limits)

    scratch_q = (
        pltpu.VMEM((2, 2 * DH, 2 * FH), BF),
        pltpu.VMEM((2 * FH, 2 * DH), BF),
        pltpu.VMEM((NTOK * HALF, 2 * DH), BF),
        pltpu.VMEM((PIECE, 2 * FH), BF),
        pltpu.SemaphoreType.DMA((NTOK,)),
    )
    answers0 = call(respond(0), shape(NTOK, HALF, 2 * DH), (role, rows1, first), 1, scratch_q, (1,))
    operands = (role, rows_q, second, answers0)
    packed = call(respond(1), shape(NTOK, OUT_ROWS, 2 * DH), operands, 1, scratch_q)
    answers, gate, up, down = call(
        unpack, (shape(2, ROWS, HEADS * DH),) + (shape(HEADS, UNITS, DH),) * 3, (exchange(packed),)
    )
    return (answers[None], *(jnp.transpose(w, (0, 2, 1))[None] for w in (gate, up, down)))


def solution(mesh):
    tokens = P("block", None, "tok", None)
    share = P("block", None, None, "tok")
    return jax.shard_map(
        program,
        mesh=mesh,
        in_specs=(tokens,) * 5 + (P(),) + (share,) * 3 + (P(),) * 3,
        out_specs=(tokens, share, share, share),
        check_vma=False,
    )
```

```python
import jax
import jax.numpy as jnp
from jax import lax
from jax.experimental import pallas as pl
from jax.experimental.pallas import tpu as pltpu
from jax.sharding import PartitionSpec as P


EPS = 1e-06
BF = jnp.bfloat16
F32 = jnp.float32

HEADS = 20
DH = 64
FH = 512
ROWS = 256
NTOK = 32
UNITS = FH // NTOK
PAIRS = HEADS // 2
EDGE = 176
MID = ROWS - EDGE
SUB = 16
TILE = 512
SHARE = 2 * UNITS
IN_ROWS = 224
MID_BLOCKS = (1, 4, 7, 10, 13)
EDGE_BLOCKS = tuple(b for b in range(ROWS // SUB) if b not in MID_BLOCKS)
HALF = EDGE // 2
OUT_ROWS = 2 * HALF + SHARE
WIDTH = 256
PIECE = 256
PACKED = NTOK * EDGE + TILE
UPS = [(3 * g + a, 3 * g + a + 1) for g in range(PAIRS) for a in (0, 1)]
DOWNS = [(3 * g + a + 1, 3 * g + a) for g in range(PAIRS) for a in (0, 1)]


def low_lanes(shape):
    return lax.broadcasted_iota(jnp.int32, shape, 1) < DH


def swap(x):
    return pltpu.roll(x.astype(F32), DH, 1).astype(x.dtype)


def pair_up(left, right):
    low = low_lanes(left.shape)
    return jnp.where(low, left, swap(right)), jnp.where(low, swap(left), right)


def scatter_rows(out_ref, g, first, second):
    for j, b in enumerate(EDGE_BLOCKS):
        to, of = slice(j * SUB, (j + 1) * SUB), slice(b * SUB, (b + 1) * SUB)
        out_ref[3 * g, to] = first[of]
        out_ref[3 * g + 2, to] = second[of]
    for j, b in enumerate(MID_BLOCKS):
        of = slice(b * SUB, (b + 1) * SUB)
        out_ref[3 * g + 1, j * SUB : (j + 1) * SUB] = first[of]
        out_ref[3 * g + 1, MID + j * SUB : MID + (j + 1) * SUB] = second[of]


def spread_of():
    owner = lax.broadcasted_iota(jnp.int32, (HEADS, HEADS * DH), 1) // DH
    return (owner == lax.broadcasted_iota(jnp.int32, (HEADS, HEADS * DH), 0)).astype(F32).astype(BF)


def scaled_values(values, rates_ref, counts_ref, stagger_ref, tick):
    offset = lax.broadcasted_iota(jnp.int32, (1, ROWS), 1)
    scale = []
    for h in range(HEADS):
        inside = (offset - stagger_ref[h] + ROWS) & (ROWS - 1)
        scale.append(jnp.where(inside < counts_ref[tick, h], rates_ref[h, tick : tick + 1].astype(F32), 0.0))
    scale = jnp.concatenate(scale, axis=0).astype(BF)
    wide = lax.dot_general(scale, spread_of(), (((0,), (0,)), ((), ())), preferred_element_type=F32)
    return (values.astype(F32) * wide).astype(BF)


def pack_first(
    counts_ref, stagger_ref, keys_hbm, values_hbm, rates_hbm, gate_hbm, up_hbm, down_hbm, out_hbm,
    keys_ref, values_ref, rates_ref, gate_ref, up_ref, down_ref, out_ref, loads, stores,
):
    pairs = (
        (rates_hbm, rates_ref),
        (values_hbm.at[0], values_ref),
        (keys_hbm.at[0], keys_ref),
        (gate_hbm, gate_ref),
        (up_hbm, up_ref),
        (down_hbm, down_ref),
    )
    copies = [pltpu.make_async_copy(src, dst, loads.at[n]) for n, (src, dst) in enumerate(pairs)]
    for copy in copies:
        copy.start()
    out_ref[3 * PAIRS :] = jnp.zeros((NTOK - 3 * PAIRS, IN_ROWS, 2 * DH), BF)
    for g in range(PAIRS):
        for d in (0, 2):
            out_ref[3 * g + d, EDGE + SHARE :] = jnp.zeros((IN_ROWS - EDGE - SHARE, 2 * DH), BF)
    for copy in copies:
        copy.wait()
    scaled = scaled_values(values_ref[...], rates_ref, counts_ref, stagger_ref, 0)

    def share(h):
        half = (UNITS // 2, DH)
        counts = [jnp.full(half, counts_ref[t, h].astype(F32), F32) for t in range(2)]
        gu = jnp.concatenate([gate_ref[h], up_ref[h]], axis=1)
        w = jnp.concatenate([jnp.concatenate(counts, axis=0).astype(BF), down_ref[h]], axis=1)
        return jnp.concatenate([gu, w], axis=0)

    sent = []
    for g in range(PAIRS + 1):
        lo, n = 3 * g, 3 if g < PAIRS else NTOK - 3 * PAIRS
        if g < PAIRS:
            lanes = slice(2 * DH * g, 2 * DH * (g + 1))
            first, second = pair_up(keys_ref[:, lanes], scaled[:, lanes])
            scatter_rows(out_ref, g, first, second)
            shares = share(2 * g), share(2 * g + 1)
            out_ref[3 * g, EDGE : EDGE + SHARE] = shares[0]
            out_ref[3 * g + 1, 2 * MID : 2 * MID + SHARE] = shares[0]
            out_ref[3 * g + 1, 2 * MID + SHARE : 2 * MID + 2 * SHARE] = shares[1]
            out_ref[3 * g + 2, EDGE : EDGE + SHARE] = shares[1]
        sent.append(pltpu.make_async_copy(out_ref.at[pl.ds(lo, n)], out_hbm.at[pl.ds(lo, n)], stores.at[g]))
        sent[-1].start()
    for copy in sent:
        copy.wait()


def pack_queries(queries, out_ref, at):
    out_ref[3 * PAIRS :, at : at + HALF] = jnp.zeros((NTOK - 3 * PAIRS, HALF, 2 * DH), BF)
    for g in range(PAIRS):
        tile = queries[:, 2 * DH * g : 2 * DH * (g + 1)].astype(F32)
        turn = pltpu.roll(tile, DH, 1)
        low = low_lanes((HALF, 2 * DH))
        out_ref[3 * g, at : at + HALF] = jnp.where(low, tile[:HALF], turn[HALF:EDGE]).astype(BF)
        middle = jnp.where(low_lanes((MID, 2 * DH)), tile[EDGE:], tile[:MID]).astype(BF)
        out_ref[3 * g + 1, at : at + MID] = middle
        out_ref[3 * g + 1, at + MID : at + HALF] = jnp.zeros((HALF - MID, 2 * DH), BF)
        out_ref[3 * g + 2, at : at + HALF] = jnp.where(low, turn[MID : MID + HALF], tile[MID + HALF :]).astype(BF)


def pack_second(counts_ref, stagger_ref, keys_ref, values_ref, rates_ref, queries_ref, out_ref):
    scaled = scaled_values(values_ref[1], rates_ref, counts_ref, stagger_ref, 1)
    keys = keys_ref[1]
    out_ref[3 * PAIRS :, :EDGE] = jnp.zeros((NTOK - 3 * PAIRS, EDGE, 2 * DH), BF)
    for g in range(PAIRS):
        out_ref[3 * g + 1, 2 * MID : EDGE] = jnp.zeros((EDGE - 2 * MID, 2 * DH), BF)
        lanes = slice(2 * DH * g, 2 * DH * (g + 1))
        scatter_rows(out_ref, g, *pair_up(keys[:, lanes], scaled[:, lanes]))
    pack_queries(queries_ref[0], out_ref, EDGE)


def pack_third(queries_ref, out_ref):
    pack_queries(queries_ref[1], out_ref, 0)


def whole_weights(role_ref, rows_hbm, out_ref, counts_ref, rows_ref, sem):
    copy = pltpu.make_async_copy(rows_hbm.at[:, pl.ds(2 * MID, 2 * SHARE)], rows_ref, sem)
    copy.start()
    role = role_ref[0]
    copy.wait()
    for slot in range(2):
        start = pl.multiple_of(jnp.where(role == 1, slot * SHARE, EDGE - 2 * MID), SUB)
        gu = jnp.concatenate([rows_ref[s, pl.ds(start, UNITS)] for s in range(NTOK)], axis=0)
        w = jnp.concatenate([rows_ref[s, pl.ds(start + UNITS, UNITS)] for s in range(NTOK)], axis=0)
        gu = gu.astype(F32).T.astype(BF)
        w = w.astype(F32).T
        out_ref[slot] = jnp.concatenate([gu[:DH], gu[DH:], w[DH:].astype(BF)], axis=1)
        counts_ref[slot : slot + 1] = w[0:1].astype(jnp.int32)


def gradient(tick):
    def kernel(
        role_ref, counts_ref, stagger_ref, rows_hbm, weights_ref, own_ref, up_ref, down_ref,
        stack, acc, packed, steps, total_ref, rows_ref, sem,
    ):
        copy = pltpu.make_async_copy(rows_hbm.at[:, pl.ds(0, EDGE)], rows_ref, sem)
        copy.start()
        role, pair = role_ref[0], role_ref[1]
        zero = jnp.zeros((DH, FH), BF)

        def step(base, tile):
            kv = packed[pl.ds(pl.multiple_of(base, SUB), tile)]
            turn = kv.T
            k_t, v_t = turn[:DH], turn[DH:]
            piece = min(PIECE, tile)
            for f in range(0, FH, WIDTH):
                for m in range(0, tile, piece):
                    x = kv[m : m + piece]
                    half_gate = jnp.dot(x, stack[:, f : f + WIDTH], preferred_element_type=F32)
                    up = jnp.dot(x, stack[:, FH + f : FH + f + WIDTH], preferred_element_type=F32)
                    back = jnp.dot(x, stack[:, 2 * FH + f : 2 * FH + f + WIDTH], preferred_element_type=F32)
                    twice = jnp.tanh(half_gate) + 1.0
                    act = half_gate * twice
                    sig = 0.5 * twice
                    slope = sig + act * (1.0 - sig)
                    at = slice(m, m + piece)
                    steps[at, f : f + WIDTH] = (back * up * slope).astype(BF)
                    steps[at, FH + f : FH + f + WIDTH] = (back * act).astype(BF)
                    steps[at, 2 * FH + f : 2 * FH + f + WIDTH] = (act * up).astype(BF)
            for f in range(0, 3 * FH, WIDTH):
                left = k_t if f < 2 * FH else v_t
                acc[:, f : f + WIDTH] += jnp.dot(left, steps[:tile, f : f + WIDTH], preferred_element_type=F32)

        def head(slot, begin, blocks):
            w = weights_ref[slot]
            half = (w[:, :FH].astype(F32) * 0.5).astype(BF)
            stack[:DH] = jnp.concatenate([half, w[:, FH : 2 * FH], zero], axis=1)
            stack[DH:] = jnp.concatenate([zero, zero, w[:, 2 * FH :]], axis=1)
            acc[...] = jnp.zeros((DH, 3 * FH), F32)
            start = stagger_ref[2 * pair + slot]
            lead = start // SUB

            def from_shard(s, n):
                limit = counts_ref[slot, s * UNITS + tick * (UNITS // 2)]
                last = (start + limit - 1) // SUB
                used = ((2 << (last - lead)) - 1) << lead
                used = used | (used >> (ROWS // SUB))
                for j, b in enumerate(blocks):
                    packed[pl.ds(pl.multiple_of(n, SUB), SUB)] = rows_ref[s, pl.ds(begin + j * SUB, SUB)]
                    n = n + ((used >> b) & 1) * SUB
                return n

            count = lax.fori_loop(0, NTOK, from_shard, jnp.int32(0))
            packed[pl.ds(pl.multiple_of(count, SUB), TILE)] = jnp.zeros((TILE, 2 * DH), BF)
            total_ref[0] = count

        def run(slot):
            count = total_ref[0]
            whole = count // TILE
            rest = count - whole * TILE
            whole = whole + jnp.where(rest > TILE // 2, 1, 0)

            def one(i, c):
                step(i * TILE, TILE)
                return c

            lax.fori_loop(0, whole, one, 0)

            @pl.when((rest > 0) & (rest <= TILE // 2))
            def _():
                step(whole * TILE, TILE // 2)

            own_ref[slot] = acc[...].astype(BF)

        copy.wait()

        def both(slot, c):
            @pl.when(role == 1)
            def _():
                head(slot, pl.multiple_of(slot * MID, SUB), MID_BLOCKS)

            @pl.when(role != 1)
            def _():
                head(slot, 0, EDGE_BLOCKS)

            run(slot)
            return c

        lax.fori_loop(jnp.where(role == 2, 1, 0), jnp.where(role == 0, 1, jnp.where(role == 3, 0, 2)), both, 0)
        up_ref[...] = own_ref[jnp.where(role == 0, 0, 1)]
        down_ref[...] = own_ref[jnp.where(role == 1, 0, 1)]

    return kernel


def renew(role_ref, weights_ref, own_ref, below_ref, above_ref, out_ref):
    role = role_ref[0]
    below, above = below_ref[...].astype(F32), above_ref[...].astype(F32)
    others = (jnp.where(role == 0, above, below), jnp.where(role == 1, above, below))
    for slot in range(2):
        base = weights_ref[slot].astype(F32)
        moved = base + (own_ref[slot].astype(F32) + others[slot])
        before = jnp.sum(base * base, axis=0, keepdims=True) + EPS
        after = jnp.sum(moved * moved, axis=0, keepdims=True) + EPS
        out_ref[slot] = (moved * (jnp.sqrt(before) / jnp.sqrt(after))).astype(BF)


def respond(tick):
    def kernel(role_ref, rows_ref, weights_ref, *refs):
        if tick == 0:
            prev_ref, (out_ref, stack, down, packed, hidden, loads) = None, refs
        else:
            prev_ref, out_ref, stack, down, packed, hidden, loads = refs
        role = role_ref[0]
        copies = []
        for s in range(NTOK):
            if tick == 1:
                packed[s * HALF : (s + 1) * HALF] = rows_ref[s]
                continue
            target = packed.at[pl.ds(s * HALF, HALF)]
            copies.append(pltpu.make_async_copy(rows_ref.at[s, pl.ds(EDGE, HALF)], target, loads.at[s]))
            copies[-1].start()
        nothing = jnp.zeros((DH, FH), F32)
        for side in range(2):
            w = weights_ref[jnp.where(role == 2, 1, jnp.where(role == 1, side, 0))]
            half = (w[:, :FH].astype(F32) * 0.5).astype(BF)
            mine = jnp.concatenate([half, w[:, FH : 2 * FH]], axis=1)
            stack[side, side * DH : (side + 1) * DH] = mine
            stack[side, (1 - side) * DH : (2 - side) * DH] = jnp.zeros((DH, 2 * FH), BF)
            back = w[:, 2 * FH :].astype(F32)
            turn = jnp.concatenate([back, nothing] if side == 0 else [nothing, back], axis=0).T.astype(BF)
            down[side * FH : (side + 1) * FH] = turn
        for copy in copies:
            copy.wait()

        def step(i, c):
            tile = pl.ds(pl.multiple_of(i * PIECE, PIECE), PIECE)
            q = packed[tile]
            for side in range(2):
                for f in range(0, FH, WIDTH):
                    half_gate = jnp.dot(q, stack[side, :, f : f + WIDTH], preferred_element_type=F32)
                    up = jnp.dot(q, stack[side, :, FH + f : FH + f + WIDTH], preferred_element_type=F32)
                    value = half_gate * (jnp.tanh(half_gate) + 1.0) * up
                    hidden[:, side * FH + f : side * FH + f + WIDTH] = value.astype(BF)
            packed[tile] = jnp.dot(hidden[...], down[...], preferred_element_type=F32).astype(BF)
            return c

        lax.fori_loop(0, NTOK * HALF // PIECE, step, 0)
        at = tick * HALF
        for s in range(NTOK):
            out_ref[s, at : at + HALF] = packed[s * HALF : (s + 1) * HALF]
        if tick == 1:
            w = jnp.where(role == 0, weights_ref[0].astype(F32), weights_ref[1].astype(F32))
            gu = jnp.concatenate([w[:, :FH], w[:, FH : 2 * FH]], axis=0).T.astype(BF)
            dn = jnp.concatenate([w[:, 2 * FH :], nothing], axis=0).T.astype(BF)
            for s in range(NTOK):
                out_ref[s, :HALF] = prev_ref[s]
                out_ref[s, 2 * HALF : 2 * HALF + UNITS] = gu[s * UNITS : (s + 1) * UNITS]
                out_ref[s, 2 * HALF + UNITS :] = dn[s * UNITS : (s + 1) * UNITS]

    return kernel


def unpack(rows_ref, answers_ref, gate_ref, up_ref, down_ref):
    for g in range(PAIRS):
        lanes = slice(2 * DH * g, 2 * DH * (g + 1))
        for t in range(2):
            one, mid, two = (rows_ref[3 * g + d, t * HALF : (t + 1) * HALF].astype(F32) for d in range(3))
            first = jnp.concatenate([one, pltpu.roll(one, DH, 1), mid[:MID]], axis=0)
            second = jnp.concatenate([mid[:MID], pltpu.roll(two, DH, 1), two], axis=0)
            answers_ref[t, :, lanes] = jnp.where(low_lanes(first.shape), first, second).astype(BF)
        for h in range(2):
            share = rows_ref[3 * g + 2 * h, 2 * HALF :]
            gate_ref[2 * g + h] = share[:UNITS, :DH]
            up_ref[2 * g + h] = swap(share[:UNITS])[:, :DH]
            down_ref[2 * g + h] = share[UNITS:, :DH]


def call(kernel, outs, args, scalars=0, scratch=(), remote=(), far=False):
    places = [pltpu.SMEM if n < scalars else pltpu.HBM if n in remote else pltpu.VMEM for n in range(len(args))]
    args = [pltpu.with_memory_space_constraint(a, p) if p == pltpu.HBM else a for a, p in zip(args, places)]
    many = isinstance(outs, (tuple, list))
    out = lambda: pl.BlockSpec(memory_space=pltpu.HBM if far else pltpu.VMEM)
    if far:
        outs = pltpu.HBM(outs.shape, outs.dtype)
    return pl.pallas_call(
        kernel,
        out_shape=outs,
        in_specs=[pl.BlockSpec(memory_space=p) for p in places],
        out_specs=tuple(out() for _ in outs) if many else out(),
        scratch_shapes=list(scratch),
        compiler_params=pltpu.CompilerParams(vmem_limit_bytes=24 * 1024 * 1024),
    )(*args)


def shape(*dims):
    return jax.ShapeDtypeStruct(dims, BF)


def exchange(rows):
    result = lax.all_to_all(rows.reshape(-1, 2 * DH), "tok", split_axis=0, concat_axis=0, tiled=True)
    return result.reshape(rows.shape)


def program(keys, values, queries, rates, counts, stagger, gate_in, up_in, down_in, entry_gate, entry_up, entry_down):
    me = lax.axis_index("tok")
    pair = jnp.minimum(me // 3, PAIRS - 1)
    role = jnp.stack([jnp.where(me < 3 * PAIRS, me % 3, 3), pair]).astype(jnp.int32)
    keys, values, queries = keys[0], values[0], queries[0]
    rates = jnp.transpose(rates[0], (2, 0, 1))
    counts = counts[0, :, 0]
    shares = [jnp.transpose(w[0], (0, 2, 1)) for w in (gate_in, up_in, down_in)]
    tokens = (counts, stagger, keys, values, rates)
    scratch = [pltpu.VMEM((ROWS, HEADS * DH), BF)] * 2 + [pltpu.VMEM(rates.shape, BF)]
    scratch += [pltpu.VMEM((HEADS, UNITS, DH), BF)] * 3 + [pltpu.VMEM((NTOK, IN_ROWS, 2 * DH), BF)]
    scratch += [pltpu.SemaphoreType.DMA((6,)), pltpu.SemaphoreType.DMA((PAIRS + 1,))]
    operands = (*tokens, *shares)
    packed0 = call(pack_first, shape(NTOK, IN_ROWS, 2 * DH), operands, 2, scratch, range(2, len(operands)), True)
    rows0 = exchange(packed0)
    tokens, queries, packed0 = lax.optimization_barrier((tokens, queries, packed0))
    packed1 = call(pack_second, shape(NTOK, EDGE + HALF, 2 * DH), (*tokens, queries), 2)
    packed_q = call(pack_third, shape(NTOK, HALF, 2 * DH), (queries,))
    rows0, packed1, packed_q = lax.optimization_barrier((rows0, packed1, packed_q))
    rows1 = exchange(packed1)
    entries = jnp.concatenate(
        [lax.dynamic_slice_in_dim(e, 2 * pair, 2, 0) for e in (entry_gate, entry_up, entry_down)], axis=2
    )

    weight = shape(DH, 3 * FH)
    weights = shape(2, DH, 3 * FH)
    stacked = (pltpu.VMEM((2 * DH, 3 * FH), BF), pltpu.VMEM((DH, 3 * FH), F32))
    scratch = (*stacked, pltpu.VMEM((PACKED, 2 * DH), BF), pltpu.VMEM((TILE, 3 * FH), BF), pltpu.SMEM((1,), jnp.int32))
    scratch += (pltpu.VMEM((NTOK, EDGE, 2 * DH), BF), pltpu.SemaphoreType.DMA)

    waiting = [packed_q]

    def advance(tick, rows, current, limits):
        own, up, down = call(
            gradient(tick), (weights, weight, weight), (role, limits, stagger, rows, current), 3, scratch, (3,)
        )
        if tick == 1:
            own, waiting[0] = lax.optimization_barrier((own, waiting[0]))
        below = lax.ppermute(up, "tok", UPS)
        above = lax.ppermute(down, "tok", DOWNS)
        return call(renew, weights, (role, current, own, below, above), 1)

    current, limits = call(
        whole_weights,
        (weights, jax.ShapeDtypeStruct((2, FH), jnp.int32)),
        (role, rows0),
        1,
        (pltpu.VMEM((NTOK, 2 * SHARE, 2 * DH), BF), pltpu.SemaphoreType.DMA),
        (1,),
    )
    first = advance(0, rows0, current, limits)
    size = lax.axis_size("block")
    passed = lax.ppermute(first, "block", [(b, b + 1) for b in range(size - 1)])
    second = advance(1, rows1, jnp.where(lax.axis_index("block") == 0, entries, passed), limits)

    rows_q = exchange(waiting[0])
    scratch_q = (
        pltpu.VMEM((2, 2 * DH, 2 * FH), BF),
        pltpu.VMEM((2 * FH, 2 * DH), BF),
        pltpu.VMEM((NTOK * HALF, 2 * DH), BF),
        pltpu.VMEM((PIECE, 2 * FH), BF),
        pltpu.SemaphoreType.DMA((NTOK,)),
    )
    answers0 = call(respond(0), shape(NTOK, HALF, 2 * DH), (role, rows1, first), 1, scratch_q, (1,))
    operands = (role, rows_q, second, answers0)
    packed = call(respond(1), shape(NTOK, OUT_ROWS, 2 * DH), operands, 1, scratch_q)
    answers, gate, up, down = call(
        unpack, (shape(2, ROWS, HEADS * DH),) + (shape(HEADS, UNITS, DH),) * 3, (exchange(packed),)
    )
    return (answers[None], *(jnp.transpose(w, (0, 2, 1))[None] for w in (gate, up, down)))


def solution(mesh):
    tokens = P("block", None, "tok", None)
    share = P("block", None, None, "tok")
    return jax.shard_map(
        program,
        mesh=mesh,
        in_specs=(tokens,) * 5 + (P(),) + (share,) * 3 + (P(),) * 3,
        out_specs=(tokens, share, share, share),
        check_vma=False,
    )
```
